32 devices in a mesh: robot: 8 (over z, x), sub: 4 (over y, core).
Axes of the slice: x: 2, y: 2, z: 4, core: 2. Of those that a mesh axis runs over, the one named last changes fastest.
Arguments:
- landmark_copies: float32 [8, 4, 3, 512], P('robot', 'sub'), may hold values from -6 to 6
- dual_copies: float32 [8, 4, 3, 512], P('robot', 'sub'), may hold values from -4 to 4
- visibility: int32 [8, 4, 512], P('robot', 'sub'), may hold values from 0 to 511
- block_counts: int32 [8, 4, 8], P('robot', 'sub'), may hold values from 1 to 64, as said below
- consensus_old: float32 [8, 4, 3, 512], P('robot', 'sub'), may hold values from -6 to 6
- poses: float32 [8, 4, 6, 1024], P('robot', 'sub'), may hold values from -6 to 6
- inverse_blocks: float32 [8, 4, 36, 1024], P('robot', 'sub'), may hold values from -1.8 to 1.8
- jacobians: float32 [8, 4, 18, 4096], P('robot', 'sub'), may hold values from -3 to 3
- measurements: float32 [8, 4, 3, 4096], P('robot', 'sub'), may hold values from -6 to 6
- obs_pose: int32 [8, 4, 4096], P('robot', 'sub'), may hold values from 0 to 1023
- obs_slot: int32 [8, 4, 4096], P('robot', 'sub'), may hold values from 0 to 511, as said below
- edge_to: int32 [8, 4, 1024], P('robot', 'sub'), may hold values from 0 to 4095
- edge_offset: float32 [8, 4, 6, 1024], P('robot', 'sub'), may hold values from -3 to 3
Outputs:
- refined_poses: float32 [8, 4, 6, 1024], P('robot', 'sub')
- consensus: float32 [8, 4, 3, 512], P('robot', 'sub')
- dual_new: float32 [8, 4, 3, 512], P('robot', 'sub')
- residual_norms: float32 [2], replicated
The draws below stay inside these ranges and needn't reach their ends.
Inputs may be any that keep to these rules, and one draw needn't show every extreme that they name: block_counts[r,s,d] counts the live slots at the head of block d; for every sub index some robot receives full blocks from every robot, which robot varies with the draw. `obs_slot`: each observation names a live slot of its own device.
All inputs are finite; a program needn't handle non-finite values.
Results may differ from the reference program's by a relative error of at most 0.0001.
Values sent between devices are 32-bit elements; how exact they have to be, the bound alone decides.
No kernel may reach another device: no remote copies, remote signals or barrier semaphores. Data moves between devices by JAX's collectives and lax.ppermute only.
A program may use at most 64 MiB of HBM per device.

```python
import math
import jax
import jax.numpy as jnp
import numpy as np
from jax import lax

LM_DEV = 512
CAP = 64
POSE_DEV = 1024
OBS_DEV = 4096
SLOTS = 512
POSES = 4096
N_ROBOT = 8
N_SUB = 4


def count_table(key):
    base = jax.random.randint(jax.random.fold_in(key, 11), (N_ROBOT, N_SUB, N_ROBOT), 1, CAP // 2 + 1)
    heavy = jax.random.randint(jax.random.fold_in(key, 12), (1, N_SUB, 1), 0, N_ROBOT)
    target = jnp.arange(N_ROBOT, dtype=jnp.int32)[None, None, :]
    return jnp.where(target == heavy, CAP, base).astype(jnp.int32)


def draw_block_counts(key, part):
    return count_table(key)


def draw_obs_slot(key, part):
    counts = count_table(key)
    blocks = jax.random.randint(jax.random.fold_in(key, 13), (N_ROBOT, N_SUB, OBS_DEV), 0, N_ROBOT)
    picks = jax.random.randint(jax.random.fold_in(key, 14), (N_ROBOT, N_SUB, OBS_DEV), 0, CAP)
    limit = jnp.take_along_axis(counts, blocks, axis=2)
    return (blocks * CAP + picks % limit).astype(jnp.int32)


def with_ends(result, rng, least, high):
    dims = result.shape
    place = [jax.random.randint(jax.random.fold_in(rng, axis), (), 0, dims[axis]) for axis in range(len(dims))]
    result = result.at[tuple(place)].set(least)
    longest = dims.index(max(dims))
    place[longest] = (place[longest] + 1) % dims[longest]
    return result.at[tuple(place)].set(high)


def block_scale(rng, extent, cuts, least, largest):
    loudness, own = 1.0, jax.random.fold_in(rng, 6)
    for axis_at, shards_of in cuts:
        heights = jnp.exp(jax.random.uniform(jax.random.fold_in(own, axis_at), (shards_of,), jnp.float32, least / len(cuts), largest / len(cuts)))
        loudness = loudness * jnp.repeat(heights, extent[axis_at] // shards_of).reshape([-1 if axis == axis_at else 1 for axis in range(len(extent))])
    return loudness


def rank_table(amount, lean):
    portions = [(1 << 20) // math.isqrt(standing ** lean) + 1 for standing in range(1, amount + 1)]
    scale = 1 + sum(portions) // (1 << 30)
    return np.cumsum(np.array([max(1, weight // scale) for weight in portions]))


def skewed_ids(rng, dims, number_of, lean):
    table = rank_table(number_of, lean)
    ticket = jax.random.randint(jax.random.fold_in(rng, 1), dims, 0, int(table[number_of - 1]))
    standing = jnp.searchsorted(jnp.asarray(table, jnp.int32), ticket, side="right")
    return jax.random.permutation(jax.random.fold_in(rng, 2), number_of)[standing].astype(jnp.int32)


def scatter_about(stream_key, extent, width, bound, split=(), kind=jnp.bfloat16):
    values = width * jax.random.normal(stream_key, extent, jnp.float32)
    if split:
        values = values * block_scale(stream_key, extent, split, -0.22, 0.18)
    return jnp.clip(values, -bound, bound).astype(kind)


def setup_inputs(seed: int = 0) -> dict:
    key_list = jax.random.split(jax.random.key(seed), 14)
    landmark_copies = scatter_about(key_list[0], (N_ROBOT, N_SUB, 3, SLOTS), 1.0, 6.0, ((0, 8), (1, 4)), jnp.float32)
    dual_copies = scatter_about(key_list[1], (N_ROBOT, N_SUB, 3, SLOTS), 0.5, 4.0, ((0, 8), (1, 4)), jnp.float32)
    visibility = with_ends(skewed_ids(key_list[2], (N_ROBOT, N_SUB, SLOTS), LM_DEV, 2), jax.random.fold_in(key_list[2], 3), 0, LM_DEV - 1).astype(jnp.int32)
    block_counts = draw_block_counts(jax.random.fold_in(key_list[13], 71), 0)
    consensus_old = scatter_about(key_list[4], (N_ROBOT, N_SUB, 3, LM_DEV), 1.0, 6.0, ((0, 8), (1, 4)), jnp.float32)
    poses = scatter_about(key_list[5], (N_ROBOT, N_SUB, 6, POSE_DEV), 1.0, 6.0, ((0, 8), (1, 4)), jnp.float32)
    inverse_blocks = scatter_about(key_list[6], (N_ROBOT, N_SUB, 36, POSE_DEV), 0.3, 1.8, ((0, 8), (1, 4)), jnp.float32)
    jacobians = scatter_about(key_list[7], (N_ROBOT, N_SUB, 18, OBS_DEV), 0.5, 3.0, ((0, 8), (1, 4)), jnp.float32)
    measurements = scatter_about(key_list[8], (N_ROBOT, N_SUB, 3, OBS_DEV), 1.0, 6.0, ((0, 8), (1, 4)), jnp.float32)
    obs_pose = with_ends(jax.random.randint(key_list[9], (N_ROBOT, N_SUB, OBS_DEV), 0, POSE_DEV), jax.random.fold_in(key_list[9], 1), 0, POSE_DEV - 1).astype(jnp.int32)
    obs_slot = draw_obs_slot(jax.random.fold_in(key_list[13], 71), 0)
    edge_to = with_ends(jax.random.randint(key_list[11], (N_ROBOT, N_SUB, POSE_DEV), 0, POSES), jax.random.fold_in(key_list[11], 1), 0, POSES - 1).astype(jnp.int32)
    edge_offset = scatter_about(key_list[12], (N_ROBOT, N_SUB, 6, POSE_DEV), 0.5, 3.0, ((0, 8), (1, 4)), jnp.float32)
    return {"landmark_copies": landmark_copies, "dual_copies": dual_copies, "visibility": visibility, "block_counts": block_counts, "consensus_old": consensus_old, "poses": poses, "inverse_blocks": inverse_blocks, "jacobians": jacobians, "measurements": measurements, "obs_pose": obs_pose, "obs_slot": obs_slot, "edge_to": edge_to, "edge_offset": edge_offset}


penalty = 2.0

def reference(landmark_copies, dual_copies, visibility, block_counts, consensus_old, poses, inverse_blocks, jacobians, measurements, obs_pose, obs_slot, edge_to, edge_offset):
    robots = N_ROBOT
    subs = N_SUB
    live_mask = (jnp.arange(CAP)[None, None, None, :] < block_counts[..., None]).reshape(robots, subs, SLOTS).astype(jnp.float32)
    outgoing = (landmark_copies + dual_copies) * live_mask[:, :, None, :]
    target = (jnp.arange(SLOTS, dtype=jnp.int32) // CAP)[None, None, :] * LM_DEV + visibility
    sum_list = []
    seen_list = []
    for sub_index in range(subs):
        values = jnp.moveaxis(outgoing[:, sub_index], 1, 0).reshape(3, robots * SLOTS)
        flat_ids = target[:, sub_index].reshape(robots * SLOTS).astype(jnp.int32)
        summed = jax.vmap(lambda entries: jax.ops.segment_sum(entries, flat_ids, num_segments=robots * LM_DEV))(values)
        sum_list.append(jnp.moveaxis(summed.reshape(3, robots, LM_DEV), 0, 1))
        counted = jax.ops.segment_sum(live_mask[:, sub_index].reshape(robots * SLOTS), flat_ids, num_segments=robots * LM_DEV)
        seen_list.append(counted.reshape(robots, LM_DEV))
    totals = jnp.stack(sum_list, axis=1)
    seen = jnp.stack(seen_list, axis=1)
    consensus = (consensus_old + totals) / (1.0 + seen[:, :, None, :])
    back_list = []
    for sub_index in range(subs):
        flat = jnp.moveaxis(consensus[:, sub_index], 1, 0).reshape(3, robots * LM_DEV)
        picked = flat[:, target[:, sub_index]]
        back_list.append(jnp.moveaxis(picked, 1, 0))
    back = jnp.stack(back_list, axis=1)
    differ = (landmark_copies - back) * live_mask[:, :, None, :]
    dual_new = dual_copies + differ
    primal = jnp.sum(differ * differ)
    change = consensus - consensus_old
    dualsum = penalty * penalty * jnp.sum(seen[:, :, None, :] * change * change)
    residual_norms = jnp.sqrt(jnp.stack([primal, dualsum]) / (LM_DEV * robots * subs))
    copies_at = jnp.take_along_axis(landmark_copies, obs_slot[:, :, None, :], axis=3)
    error = measurements - copies_at
    jac_rows = jacobians.reshape(robots, subs, 3, 6, OBS_DEV)
    pull = lax.optimization_barrier(jnp.sum(jac_rows * error[:, :, :, None, :], axis=2))

    def pose_sums(rows, pose_ids):
        return jax.vmap(lambda entries: jax.ops.segment_sum(entries, pose_ids, num_segments=POSE_DEV))(rows)
    grad_obs = jax.vmap(jax.vmap(pose_sums))(pull, obs_pose)
    robot_all = jnp.moveaxis(poses, 1, 2).reshape(robots, 6, subs * POSE_DEV)
    pose_far = jax.vmap(lambda table, where: table[:, where])(robot_all, edge_to.reshape(robots, subs * POSE_DEV))
    pose_far = jnp.moveaxis(pose_far.reshape(robots, 6, subs, POSE_DEV), 2, 1)
    grad = grad_obs + pose_far - poses - edge_offset
    inverse = inverse_blocks.reshape(robots, subs, 6, 6, POSE_DEV)
    delta = lax.optimization_barrier(jnp.sum(inverse * grad[:, :, None, :, :], axis=3))
    return (poses + delta, consensus, dual_new, residual_norms)
```

```python
import functools

import jax
import jax.numpy as jnp
from jax import lax
from jax.experimental import pallas as pl
from jax.experimental.pallas import tpu as pltpu
from jax.sharding import PartitionSpec as P

penalty = 2.0
LANES = 128
SUBLANES = 8
FIELDS = 8
SHIFT = LANES.bit_length() - 1


def split3(value):
    high = value.astype(jnp.bfloat16).astype(jnp.float32)
    rest = value - high
    middle = rest.astype(jnp.bfloat16).astype(jnp.float32)
    low = (rest - middle).astype(jnp.bfloat16).astype(jnp.float32)
    return high, middle, low


def lookup(tables, index, out_rows):
    low = index & (LANES - 1)
    high = index >> SHIFT
    results = []
    for rows in tables:
        total = None
        for k, row in enumerate(rows):
            table = jnp.broadcast_to(row, (out_rows, LANES))
            got = jnp.take_along_axis(table, low, axis=1, mode="promise_in_bounds")
            total = got if total is None else jnp.where(high == k, got, total)
        results.append(total)
    return results


def segment_rows(values, index, chunks, out_rows):
    sub = lax.broadcasted_iota(jnp.int32, (out_rows, LANES), 0)
    lane_ids = lax.broadcasted_iota(jnp.int32, (LANES, LANES), 0)
    group = min(4, chunks)
    total = None
    for start in range(0, chunks, group):
        left, right = [], []
        for t in range(start, start + group):
            ids = index(t)
            high = jnp.broadcast_to(ids >> SHIFT, (out_rows, LANES)) == sub
            low = jnp.broadcast_to(ids & (LANES - 1), (LANES, LANES)) == lane_ids
            left.append(
                jnp.concatenate(
                    [
                        jnp.where(high, jnp.broadcast_to(row, (out_rows, LANES)), 0.0)
                        for row in values(t)
                    ],
                    axis=0,
                ).astype(jnp.bfloat16)
            )
            right.append(jnp.where(low, 1.0, 0.0).astype(jnp.bfloat16))
        part = lax.dot_general(
            jnp.concatenate(left, axis=1),
            jnp.concatenate(right, axis=1),
            (((1,), (1,)), ((), ())),
            preferred_element_type=jnp.float32,
        )
        total = part if total is None else total + part
    return total


def column_of(counts_ref, first, step, rows):
    sub = lax.broadcasted_iota(jnp.int32, (rows, LANES), 0)
    result = jnp.zeros((rows, LANES), jnp.int32)
    for k in range(rows):
        result = jnp.where(sub == k, counts_ref[0, first + step * k], result)
    return result


def pack_kernel(block, counts_ref, copies_ref, duals_ref, ids_ref, out_ref):
    rows = ids_ref.shape[0]
    per = LANES // block
    lane = lax.broadcasted_iota(jnp.int32, (rows, LANES), 1)
    sources = [copies_ref[k] for k in range(3)] + [duals_ref[k] for k in range(3)]
    sources.append(ids_ref[...].astype(jnp.float32))
    for j in range(per):
        for v, source in enumerate(sources):
            moved = pltpu.roll(source, LANES - j * block, 1) if j else source
            out_ref[pl.ds(j * FIELDS + v, rows, per * FIELDS), :] = moved
        live = (lane < column_of(counts_ref, j, per, rows)).astype(jnp.float32)
        out_ref[pl.ds(j * FIELDS + 7, rows, per * FIELDS), :] = live


def owner_kernel(block, subs, recv_ref, old_ref, consensus_ref, out_ref):
    robots = recv_ref.shape[0] // FIELDS
    rows = old_ref.shape[1]
    padded = max(rows, SUBLANES)
    field = [recv_ref[pl.ds(v, robots, FIELDS), :] for v in range(FIELDS)]
    live = field[7]
    ids = field[6].astype(jnp.int32)
    pieces = [split3(live * (field[v] + field[3 + v])) for v in range(3)]
    planes = [pieces[v][s] for s in range(3) for v in range(3)] + [live]
    sums = segment_rows(
        lambda t: [plane[t : t + 1] for plane in planes],
        lambda t: ids[t : t + 1],
        robots,
        padded,
    )

    def plane_sum(j):
        return sums[j * padded : j * padded + rows]

    seen = plane_sum(9)
    weight = 1.0 + seen
    dual_sum = jnp.zeros((rows, LANES), jnp.float32)
    tables = []
    for v in range(3):
        old = old_ref[v]
        new = (old + (plane_sum(v) + (plane_sum(3 + v) + plane_sum(6 + v)))) / weight
        consensus_ref[v] = new
        change = new - old
        dual_sum = dual_sum + seen * change * change
        tables.append([new[k : k + 1] for k in range(rows)])
    back = lookup(tables, ids, robots)
    primal = jnp.zeros((robots, LANES), jnp.float32)
    for v in range(3):
        differ = (field[v] - back[v]) * live
        primal = primal + differ * differ
    primal = jnp.sum(primal, axis=(0, 1), keepdims=True)
    dual_sum = penalty * penalty * jnp.sum(dual_sum, axis=(0, 1), keepdims=True)
    lane = lax.broadcasted_iota(jnp.int32, (robots, LANES), 1)
    first = jnp.where(lane < block, back[0], pltpu.roll(back[1], block, 1))
    sums_row = jnp.where(lane == block, primal, jnp.where(lane == block + 1, dual_sum, 0.0))
    second = jnp.where(lane < block, back[2], sums_row)
    for s in range(subs):
        out_ref[pl.ds(2 * s, robots, 2 * subs), :] = first
        out_ref[pl.ds(2 * s + 1, robots, 2 * subs), :] = second


def observe_kernel(copies_ref, measured_ref, jac_ref, slot_ref, pose_ref, out_ref, planes_ref):
    rows = slot_ref.shape[0]
    table_rows = copies_ref.shape[1]
    out_rows = out_ref.shape[1]
    for start in range(0, rows, SUBLANES):
        part = pl.ds(start, SUBLANES)
        tables = [[copies_ref[k, pl.ds(j, 1), :] for j in range(table_rows)] for k in range(3)]
        at = lookup(tables, slot_ref[part, :], SUBLANES)
        error = [measured_ref[k, part, :] - at[k] for k in range(3)]
        for a in range(6):
            pull = (
                jac_ref[a, part, :] * error[0]
                + jac_ref[6 + a, part, :] * error[1]
                + jac_ref[12 + a, part, :] * error[2]
            )
            for s, piece in enumerate(split3(pull)):
                planes_ref[s * 6 + a, part, :] = piece
    sums = segment_rows(
        lambda t: [planes_ref[j, pl.ds(t, 1), :] for j in range(18)],
        lambda t: pose_ref[pl.ds(t, 1), :],
        rows,
        out_rows,
    )
    for a in range(6):
        high, middle, low = (
            sums[(s * 6 + a) * out_rows : (s * 6 + a + 1) * out_rows] for s in range(3)
        )
        out_ref[a] = high + (middle + low)


def refine_kernel(all_ref, pose_ref, grad_ref, inverse_ref, edge_ref, offset_ref, out_ref):
    subs = all_ref.shape[0]
    rows = edge_ref.shape[0]
    tables = [
        [all_ref[s, a, pl.ds(k, 1), :] for s in range(subs) for k in range(rows)] for a in range(6)
    ]
    far = lookup(tables, edge_ref[...], rows)
    grad = [grad_ref[a] + far[a] - pose_ref[a] - offset_ref[a] for a in range(6)]
    for a in range(6):
        delta = inverse_ref[a * 6] * grad[0]
        for b in range(1, 6):
            delta = delta + inverse_ref[a * 6 + b] * grad[b]
        out_ref[a] = pose_ref[a] + delta


def finish_kernel(
    block, subs, landmark_total, where_ref, counts_ref, recv_ref, copies_ref, duals_ref,
    dual_ref, norm_ref,
):
    rows = copies_ref.shape[1]
    per = LANES // block
    robots = rows * per
    me = where_ref[0]
    lane = lax.broadcasted_iota(jnp.int32, (rows, LANES), 1)
    back = [jnp.zeros((rows, LANES), jnp.float32) for _ in range(3)]
    live = jnp.zeros((rows, LANES), jnp.bool_)
    for j in range(per):
        here = (lane >= j * block) & (lane < (j + 1) * block)
        live = live | (here & (lane - j * block < column_of(counts_ref, j, per, rows)))
        for v, (line, at) in enumerate(((0, 0), (0, block), (1, 0))):
            start = 2 * (j * subs + me) + line
            got = recv_ref[pl.ds(start, rows, 2 * subs * per), :]
            turn = (j * block - at) % LANES
            moved = pltpu.roll(got, turn, 1) if turn else got
            back[v] = jnp.where(here, moved, back[v])
    for v in range(3):
        differ = jnp.where(live, copies_ref[v] - back[v], 0.0)
        dual_ref[v] = duals_ref[v] + differ
    sums = jnp.sum(recv_ref[pl.ds(1, robots * subs, 2), :], axis=0, keepdims=True)
    norms = jnp.sqrt(sums / landmark_total)
    lane = lax.broadcasted_iota(jnp.int32, (1, LANES), 1)
    for k in range(2):
        norm_ref[k] = jnp.sum(jnp.where(lane == block + k, norms, 0.0))


VMEM = pl.BlockSpec(memory_space=pltpu.VMEM)
SMEM = pl.BlockSpec(memory_space=pltpu.SMEM)


def call(kernel, outs, in_specs, name, out_specs=None, scratch=()):
    shapes = [jax.ShapeDtypeStruct(shape, jnp.float32) for shape in outs]
    return pl.pallas_call(
        kernel,
        out_shape=shapes,
        in_specs=in_specs,
        out_specs=out_specs or [VMEM] * len(outs),
        scratch_shapes=list(scratch),
        name=name,
    )


def body(
    landmark_copies,
    dual_copies,
    visibility,
    block_counts,
    consensus_old,
    poses,
    inverse_blocks,
    jacobians,
    measurements,
    obs_pose,
    obs_slot,
    edge_to,
    edge_offset,
):
    robots = lax.axis_size("robot")
    subs = lax.axis_size("sub")
    slots = landmark_copies.shape[3]
    owned = consensus_old.shape[3]
    pose_count = poses.shape[3]
    observed = obs_slot.shape[2]
    block = slots // robots
    rows, owned_rows = slots // LANES, owned // LANES
    pose_rows, obs_rows = pose_count // LANES, observed // LANES

    copies = landmark_copies.reshape(3, rows, LANES)
    duals = dual_copies.reshape(3, rows, LANES)
    ids = visibility.reshape(rows, LANES)
    counts = block_counts.reshape(1, robots)
    old = consensus_old.reshape(3, owned_rows, LANES)
    pose_block = poses.reshape(6, pose_rows, LANES)
    inverse = inverse_blocks.reshape(36, pose_rows, LANES)
    jac = jacobians.reshape(18, obs_rows, LANES)
    measured = measurements.reshape(3, obs_rows, LANES)
    pose_ids = obs_pose.reshape(obs_rows, LANES)
    slot_ids = obs_slot.reshape(obs_rows, LANES)
    edges = edge_to.reshape(pose_rows, LANES)
    offset = edge_offset.reshape(6, pose_rows, LANES)

    (outgoing,) = call(
        functools.partial(pack_kernel, block),
        [(robots * FIELDS, LANES)],
        [SMEM, VMEM, VMEM, VMEM],
        "pack",
    )(counts, copies, duals, ids)
    received = lax.all_to_all(
        outgoing.reshape(robots, FIELDS, LANES), "robot", 0, 0, tiled=True
    ).reshape(robots * FIELDS, LANES)

    everyone = lax.all_to_all(
        jnp.broadcast_to(pose_block[None], (subs, 6, pose_rows, LANES)), "sub", 0, 0, tiled=True
    )
    (grad_obs,) = call(
        observe_kernel,
        [(6, pose_rows, LANES)],
        [VMEM] * 5,
        "observe",
        scratch=[pltpu.VMEM((18, obs_rows, LANES), jnp.float32)],
    )(copies, measured, jac, slot_ids, pose_ids)

    consensus, returning = call(
        functools.partial(owner_kernel, block, subs),
        [(3, owned_rows, LANES), (robots * subs * 2, LANES)],
        [VMEM, VMEM],
        "owner",
    )(received, old)
    back = lax.all_to_all(
        returning.reshape(robots * subs, 2, LANES), ("robot", "sub"), 0, 0, tiled=True
    ).reshape(robots * subs * 2, LANES)

    (refined,) = call(
        refine_kernel, [(6, pose_rows, LANES)], [VMEM] * 6, "refine"
    )(everyone, pose_block, grad_obs, inverse, edges, offset)

    where = lax.axis_index("sub").astype(jnp.int32).reshape(1)
    dual_new, residual_norms = call(
        functools.partial(finish_kernel, block, subs, float(owned * robots * subs)),
        [(3, rows, LANES), (2,)],
        [SMEM, SMEM, VMEM, VMEM, VMEM],
        "finish",
        out_specs=[VMEM, SMEM],
    )(where, counts, back, copies, duals)
    return (
        refined.reshape(1, 1, 6, pose_count),
        consensus.reshape(1, 1, 3, owned),
        dual_new.reshape(1, 1, 3, slots),
        residual_norms,
    )


def solution(mesh):
    split4 = P("robot", "sub", None, None)
    split3d = P("robot", "sub", None)
    return jax.shard_map(
        body,
        mesh=mesh,
        in_specs=(
            split4,
            split4,
            split3d,
            split3d,
            split4,
            split4,
            split4,
            split4,
            split4,
            split3d,
            split3d,
            split3d,
            split4,
        ),
        out_specs=(split4, split4, split4, P()),
        check_vma=False,
    )
```

```python
import functools

import jax
import jax.numpy as jnp
from jax import lax
from jax.experimental import pallas as pl
from jax.experimental.pallas import tpu as pltpu
from jax.sharding import PartitionSpec as P


penalty = 2.0
LANES = 128
SUBLANES = 8
FIELDS = 8
SHIFT = LANES.bit_length() - 1


def split3(value):
    high = value.astype(jnp.bfloat16).astype(jnp.float32)
    rest = value - high
    middle = rest.astype(jnp.bfloat16).astype(jnp.float32)
    low = (rest - middle).astype(jnp.bfloat16).astype(jnp.float32)
    return high, middle, low


def lookup(tables, index, out_rows):
    low = index & (LANES - 1)
    high = index >> SHIFT
    results = []
    for rows in tables:
        total = None
        for k, row in enumerate(rows):
            table = jnp.broadcast_to(row, (out_rows, LANES))
            got = jnp.take_along_axis(table, low, axis=1, mode="promise_in_bounds")
            total = got if total is None else jnp.where(high == k, got, total)
        results.append(total)
    return results


def segment_rows(values, index, chunks, out_rows):
    sub = lax.broadcasted_iota(jnp.int32, (out_rows, LANES), 0)
    lane_ids = lax.broadcasted_iota(jnp.int32, (LANES, LANES), 0)
    group = min(4, chunks)
    total = None
    for start in range(0, chunks, group):
        left, right = [], []
        for t in range(start, start + group):
            ids = index(t)
            high = jnp.broadcast_to(ids >> SHIFT, (out_rows, LANES)) == sub
            low = jnp.broadcast_to(ids & (LANES - 1), (LANES, LANES)) == lane_ids
            left.append(
                jnp.concatenate(
                    [
                        jnp.where(high, jnp.broadcast_to(row, (out_rows, LANES)), 0.0)
                        for row in values(t)
                    ],
                    axis=0,
                ).astype(jnp.bfloat16)
            )
            right.append(jnp.where(low, 1.0, 0.0).astype(jnp.bfloat16))
        part = lax.dot_general(
            jnp.concatenate(left, axis=1),
            jnp.concatenate(right, axis=1),
            (((1,), (1,)), ((), ())),
            preferred_element_type=jnp.float32,
        )
        total = part if total is None else total + part
    return total


def column_of(counts_ref, first, step, rows):
    sub = lax.broadcasted_iota(jnp.int32, (rows, LANES), 0)
    result = jnp.zeros((rows, LANES), jnp.int32)
    for k in range(rows):
        result = jnp.where(sub == k, counts_ref[0, first + step * k], result)
    return result


def pack_kernel(block, counts_ref, copies_ref, duals_ref, ids_ref, out_ref):
    rows = ids_ref.shape[0]
    per = LANES // block
    lane = lax.broadcasted_iota(jnp.int32, (rows, LANES), 1)
    sources = [copies_ref[k] for k in range(3)] + [duals_ref[k] for k in range(3)]
    sources.append(ids_ref[...].astype(jnp.float32))
    for j in range(per):
        for v, source in enumerate(sources):
            moved = pltpu.roll(source, LANES - j * block, 1) if j else source
            out_ref[pl.ds(j * FIELDS + v, rows, per * FIELDS), :] = moved
        live = (lane < column_of(counts_ref, j, per, rows)).astype(jnp.float32)
        out_ref[pl.ds(j * FIELDS + 7, rows, per * FIELDS), :] = live


def owner_kernel(block, subs, recv_ref, old_ref, consensus_ref, out_ref):
    robots = recv_ref.shape[0] // FIELDS
    rows = old_ref.shape[1]
    padded = max(rows, SUBLANES)
    field = [recv_ref[pl.ds(v, robots, FIELDS), :] for v in range(FIELDS)]
    live = field[7]
    ids = field[6].astype(jnp.int32)
    pieces = [split3(live * (field[v] + field[3 + v])) for v in range(3)]
    planes = [pieces[v][s] for s in range(3) for v in range(3)] + [live]
    sums = segment_rows(
        lambda t: [plane[t : t + 1] for plane in planes],
        lambda t: ids[t : t + 1],
        robots,
        padded,
    )

    def plane_sum(j):
        return sums[j * padded : j * padded + rows]

    seen = plane_sum(9)
    weight = 1.0 + seen
    dual_sum = jnp.zeros((rows, LANES), jnp.float32)
    tables = []
    for v in range(3):
        old = old_ref[v]
        new = (old + (plane_sum(v) + (plane_sum(3 + v) + plane_sum(6 + v)))) / weight
        consensus_ref[v] = new
        change = new - old
        dual_sum = dual_sum + seen * change * change
        tables.append([new[k : k + 1] for k in range(rows)])
    back = lookup(tables, ids, robots)
    primal = jnp.zeros((robots, LANES), jnp.float32)
    for v in range(3):
        differ = (field[v] - back[v]) * live
        primal = primal + differ * differ
    primal = jnp.sum(primal, axis=(0, 1), keepdims=True)
    dual_sum = penalty * penalty * jnp.sum(dual_sum, axis=(0, 1), keepdims=True)
    lane = lax.broadcasted_iota(jnp.int32, (robots, LANES), 1)
    first = jnp.where(lane < block, back[0], pltpu.roll(back[1], block, 1))
    sums_row = jnp.where(lane == block, primal, jnp.where(lane == block + 1, dual_sum, 0.0))
    second = jnp.where(lane < block, back[2], sums_row)
    for s in range(subs):
        out_ref[pl.ds(2 * s, robots, 2 * subs), :] = first
        out_ref[pl.ds(2 * s + 1, robots, 2 * subs), :] = second


def observe_kernel(copies_ref, measured_ref, jac_ref, slot_ref, pose_ref, out_ref, planes_ref):
    rows = slot_ref.shape[0]
    table_rows = copies_ref.shape[1]
    out_rows = out_ref.shape[1]
    for start in range(0, rows, SUBLANES):
        part = pl.ds(start, SUBLANES)
        tables = [[copies_ref[k, pl.ds(j, 1), :] for j in range(table_rows)] for k in range(3)]
        at = lookup(tables, slot_ref[part, :], SUBLANES)
        error = [measured_ref[k, part, :] - at[k] for k in range(3)]
        for a in range(6):
            pull = (
                jac_ref[a, part, :] * error[0]
                + jac_ref[6 + a, part, :] * error[1]
                + jac_ref[12 + a, part, :] * error[2]
            )
            for s, piece in enumerate(split3(pull)):
                planes_ref[s * 6 + a, part, :] = piece
    sums = segment_rows(
        lambda t: [planes_ref[j, pl.ds(t, 1), :] for j in range(18)],
        lambda t: pose_ref[pl.ds(t, 1), :],
        rows,
        out_rows,
    )
    for a in range(6):
        high, middle, low = (
            sums[(s * 6 + a) * out_rows : (s * 6 + a + 1) * out_rows] for s in range(3)
        )
        out_ref[a] = high + (middle + low)


def refine_kernel(where_ref, edge_ref, grad_ref, inverse_ref, offset_ref, *refs):
    blocks, out_ref = refs[:-1], refs[-1]
    pose_ref = blocks[0]
    subs = len(blocks)
    rows = edge_ref.shape[0]
    count = rows * LANES
    edge = edge_ref[...]
    place = lax.rem(where_ref[0] + subs - edge // count, subs)
    tables = [
        [held[a, pl.ds(k, 1), :] for held in blocks for k in range(rows)] for a in range(6)
    ]
    far = lookup(tables, place * count + lax.rem(edge, count), rows)
    grad = [grad_ref[a] + far[a] - pose_ref[a] - offset_ref[a] for a in range(6)]
    for a in range(6):
        delta = inverse_ref[a * 6] * grad[0]
        for b in range(1, 6):
            delta = delta + inverse_ref[a * 6 + b] * grad[b]
        out_ref[a] = pose_ref[a] + delta


def finish_kernel(
    block, subs, landmark_total, where_ref, counts_ref, recv_ref, copies_ref, duals_ref,
    dual_ref, norm_ref,
):
    rows = copies_ref.shape[1]
    per = LANES // block
    robots = rows * per
    me = where_ref[0]
    lane = lax.broadcasted_iota(jnp.int32, (rows, LANES), 1)
    back = [jnp.zeros((rows, LANES), jnp.float32) for _ in range(3)]
    live = jnp.zeros((rows, LANES), jnp.bool_)
    for j in range(per):
        here = (lane >= j * block) & (lane < (j + 1) * block)
        live = live | (here & (lane - j * block < column_of(counts_ref, j, per, rows)))
        for v, (line, at) in enumerate(((0, 0), (0, block), (1, 0))):
            start = 2 * (j * subs + me) + line
            got = recv_ref[pl.ds(start, rows, 2 * subs * per), :]
            turn = (j * block - at) % LANES
            moved = pltpu.roll(got, turn, 1) if turn else got
            back[v] = jnp.where(here, moved, back[v])
    for v in range(3):
        differ = jnp.where(live, copies_ref[v] - back[v], 0.0)
        dual_ref[v] = duals_ref[v] + differ
    sums = jnp.sum(recv_ref[pl.ds(1, robots * subs, 2), :], axis=0, keepdims=True)
    norms = jnp.sqrt(sums / landmark_total)
    lane = lax.broadcasted_iota(jnp.int32, (1, LANES), 1)
    for k in range(2):
        norm_ref[k] = jnp.sum(jnp.where(lane == block + k, norms, 0.0))


VMEM = pl.BlockSpec(memory_space=pltpu.VMEM)
SMEM = pl.BlockSpec(memory_space=pltpu.SMEM)


def in_vmem(value):
    return pltpu.with_memory_space_constraint(value, pltpu.VMEM)


def call(kernel, outs, in_specs, out_specs=None, scratch=()):
    shapes = [
        jax.ShapeDtypeStruct(shape, jnp.float32) if isinstance(shape, tuple) else shape
        for shape in outs
    ]
    return pl.pallas_call(
        kernel,
        out_shape=shapes,
        in_specs=in_specs,
        out_specs=out_specs or [VMEM] * len(outs),
        scratch_shapes=list(scratch),
    )


def step(
    landmark_copies,
    dual_copies,
    visibility,
    block_counts,
    consensus_old,
    poses,
    inverse_blocks,
    jacobians,
    measurements,
    obs_pose,
    obs_slot,
    edge_to,
    edge_offset,
):
    robots = lax.axis_size("robot")
    subs = lax.axis_size("sub")
    slots = landmark_copies.shape[3]
    owned = consensus_old.shape[3]
    pose_count = poses.shape[3]
    observed = obs_slot.shape[2]
    block = slots // robots
    rows, owned_rows = slots // LANES, owned // LANES
    pose_rows, obs_rows = pose_count // LANES, observed // LANES

    copies = landmark_copies.reshape(3, rows, LANES)
    duals = dual_copies.reshape(3, rows, LANES)
    ids = visibility.reshape(rows, LANES)
    counts = block_counts.reshape(1, robots)
    old = consensus_old.reshape(3, owned_rows, LANES)
    pose_block = poses.reshape(6, pose_rows, LANES)
    inverse = inverse_blocks.reshape(36, pose_rows, LANES)
    jac = jacobians.reshape(18, obs_rows, LANES)
    measured = measurements.reshape(3, obs_rows, LANES)
    pose_ids = obs_pose.reshape(obs_rows, LANES)
    slot_ids = obs_slot.reshape(obs_rows, LANES)
    edges = edge_to.reshape(pose_rows, LANES)
    offset = edge_offset.reshape(6, pose_rows, LANES)

    where = lax.axis_index("sub").astype(jnp.int32).reshape(1)
    held = [pose_block]
    for k in range(1, subs):
        ring = [(i, (i + k) % subs) for i in range(subs)]
        held.append(lax.ppermute(pose_block, "sub", ring))

    (outgoing,) = call(
        functools.partial(pack_kernel, block),
        [pltpu.VMEM((robots * FIELDS, LANES), jnp.float32)],
        [SMEM, VMEM, VMEM, VMEM],
    )(counts, copies, duals, ids)
    received = lax.all_to_all(
        outgoing.reshape(robots, FIELDS, LANES), "robot", 0, 0, tiled=True
    ).reshape(robots * FIELDS, LANES)

    (grad_obs,) = call(
        observe_kernel,
        [pltpu.VMEM((6, pose_rows, LANES), jnp.float32)],
        [VMEM] * 5,
        scratch=[pltpu.VMEM((18, obs_rows, LANES), jnp.float32)],
    )(copies, measured, jac, slot_ids, pose_ids)

    consensus, returning = call(
        functools.partial(owner_kernel, block, subs),
        [
            pltpu.VMEM((3, owned_rows, LANES), jnp.float32),
            pltpu.VMEM((robots * subs * 2, LANES), jnp.float32),
        ],
        [VMEM, VMEM],
    )(in_vmem(received), in_vmem(old))
    back = lax.all_to_all(
        returning.reshape(robots * subs, 2, LANES), ("robot", "sub"), 0, 0, tiled=True
    ).reshape(robots * subs * 2, LANES)

    (refined,) = call(
        refine_kernel, [(6, pose_rows, LANES)], [SMEM] + [VMEM] * (4 + subs)
    )(where, edges, in_vmem(grad_obs), inverse, offset, *held)

    dual_new, residual_norms = call(
        functools.partial(finish_kernel, block, subs, float(owned * robots * subs)),
        [(3, rows, LANES), (2,)],
        [SMEM, SMEM, VMEM, VMEM, VMEM],
        out_specs=[VMEM, SMEM],
    )(where, counts, in_vmem(back), in_vmem(copies), in_vmem(duals))
    return (
        refined.reshape(1, 1, 6, pose_count),
        consensus.reshape(1, 1, 3, owned),
        dual_new.reshape(1, 1, 3, slots),
        residual_norms,
    )


def solution(mesh):
    split4 = P("robot", "sub", None, None)
    split3d = P("robot", "sub", None)
    return jax.shard_map(
        step,
        mesh=mesh,
        in_specs=(
            split4,
            split4,
            split3d,
            split3d,
            split4,
            split4,
            split4,
            split4,
            split4,
            split3d,
            split3d,
            split3d,
            split4,
        ),
        out_specs=(split4, split4, split4, P()),
        check_vma=False,
    )
```

```python
import functools

import jax
import jax.numpy as jnp
from jax import lax
from jax.experimental import pallas as pl
from jax.experimental.pallas import tpu as pltpu
from jax.sharding import PartitionSpec as P


penalty = 2.0
LANES = 128
SUBLANES = 8
FIELDS = 8
SHIFT = LANES.bit_length() - 1


def split3(value):
    high = value.astype(jnp.bfloat16).astype(jnp.float32)
    rest = value - high
    middle = rest.astype(jnp.bfloat16).astype(jnp.float32)
    low = (rest - middle).astype(jnp.bfloat16).astype(jnp.float32)
    return high, middle, low


def lookup(tables, index, out_rows):
    low = index & (LANES - 1)
    high = index >> SHIFT
    results = []
    for rows in tables:
        total = None
        for k, row in enumerate(rows):
            table = jnp.broadcast_to(row, (out_rows, LANES))
            got = jnp.take_along_axis(table, low, axis=1, mode="promise_in_bounds")
            total = got if total is None else jnp.where(high == k, got, total)
        results.append(total)
    return results


def segment_rows(values, index, chunks, out_rows):
    sub = lax.broadcasted_iota(jnp.int32, (out_rows, LANES), 0)
    lane_ids = lax.broadcasted_iota(jnp.int32, (LANES, LANES), 0)
    group = min(4, chunks)
    total = None
    for start in range(0, chunks, group):
        left, right = [], []
        for t in range(start, start + group):
            ids = index(t)
            high = jnp.broadcast_to(ids >> SHIFT, (out_rows, LANES)) == sub
            low = jnp.broadcast_to(ids & (LANES - 1), (LANES, LANES)) == lane_ids
            left.append(
                jnp.concatenate(
                    [
                        jnp.where(high, jnp.broadcast_to(row, (out_rows, LANES)), 0.0)
                        for row in values(t)
                    ],
                    axis=0,
                ).astype(jnp.bfloat16)
            )
            right.append(jnp.where(low, 1.0, 0.0).astype(jnp.bfloat16))
        part = lax.dot_general(
            jnp.concatenate(left, axis=1),
            jnp.concatenate(right, axis=1),
            (((1,), (1,)), ((), ())),
            preferred_element_type=jnp.float32,
        )
        total = part if total is None else total + part
    return total


def column_of(counts_ref, first, step, rows):
    sub = lax.broadcasted_iota(jnp.int32, (rows, LANES), 0)
    result = jnp.zeros((rows, LANES), jnp.int32)
    for k in range(rows):
        result = jnp.where(sub == k, counts_ref[0, first + step * k], result)
    return result


def pack_kernel(block, counts_ref, copies_ref, duals_ref, ids_ref, out_ref, live_ref):
    rows = ids_ref.shape[0]
    per = LANES // block
    lane = lax.broadcasted_iota(jnp.int32, (rows, LANES), 1)
    sources = [copies_ref[k] for k in range(3)] + [duals_ref[k] for k in range(3)]
    sources.append(ids_ref[...].astype(jnp.float32))
    mask = jnp.zeros((rows, LANES), jnp.float32)
    for j in range(per):
        for v, source in enumerate(sources):
            moved = pltpu.roll(source, LANES - j * block, 1) if j else source
            out_ref[pl.ds(j * FIELDS + v, rows, per * FIELDS), :] = moved
        count = column_of(counts_ref, j, per, rows)
        live = (lane < count).astype(jnp.float32)
        out_ref[pl.ds(j * FIELDS + 7, rows, per * FIELDS), :] = live
        here = (lane >= j * block) & (lane < j * block + count)
        mask = jnp.where(here, 1.0, mask)
    live_ref[...] = mask


def owner_kernel(block, subs, recv_ref, old_ref, consensus_ref, out_ref):
    robots = recv_ref.shape[0] // FIELDS
    rows = old_ref.shape[1]
    padded = max(rows, SUBLANES)
    field = [recv_ref[pl.ds(v, robots, FIELDS), :] for v in range(FIELDS)]
    live = field[7]
    ids = field[6].astype(jnp.int32)
    pieces = [split3(live * (field[v] + field[3 + v])) for v in range(3)]
    planes = [pieces[v][s] for s in range(3) for v in range(3)] + [live]
    sums = segment_rows(
        lambda t: [plane[t : t + 1] for plane in planes],
        lambda t: ids[t : t + 1],
        robots,
        padded,
    )

    def plane_sum(j):
        return sums[j * padded : j * padded + rows]

    seen = plane_sum(9)
    weight = 1.0 + seen
    dual_sum = jnp.zeros((rows, LANES), jnp.float32)
    tables = []
    for v in range(3):
        old = old_ref[v]
        new = (old + (plane_sum(v) + (plane_sum(3 + v) + plane_sum(6 + v)))) / weight
        consensus_ref[v] = new
        change = new - old
        dual_sum = dual_sum + seen * change * change
        tables.append([new[k : k + 1] for k in range(rows)])
    back = lookup(tables, ids, robots)
    primal = jnp.zeros((robots, LANES), jnp.float32)
    for v in range(3):
        differ = (field[v] - back[v]) * live
        primal = primal + differ * differ
    primal = jnp.sum(primal, axis=(0, 1), keepdims=True)
    dual_sum = penalty * penalty * jnp.sum(dual_sum, axis=(0, 1), keepdims=True)
    lane = lax.broadcasted_iota(jnp.int32, (robots, LANES), 1)
    first = jnp.where(lane < block, back[0], pltpu.roll(back[1], block, 1))
    sums_row = jnp.where(lane == block, primal, jnp.where(lane == block + 1, dual_sum, 0.0))
    second = jnp.where(lane < block, back[2], sums_row)
    for s in range(subs):
        out_ref[pl.ds(2 * s, robots, 2 * subs), :] = first
        out_ref[pl.ds(2 * s + 1, robots, 2 * subs), :] = second


def observe_kernel(copies_ref, measured_ref, jac_ref, slot_ref, pose_ref, out_ref, planes_ref):
    rows = slot_ref.shape[0]
    table_rows = copies_ref.shape[1]
    out_rows = out_ref.shape[1]
    for start in range(0, rows, SUBLANES):
        part = pl.ds(start, SUBLANES)
        tables = [[copies_ref[k, pl.ds(j, 1), :] for j in range(table_rows)] for k in range(3)]
        at = lookup(tables, slot_ref[part, :], SUBLANES)
        error = [measured_ref[k, part, :] - at[k] for k in range(3)]
        for a in range(6):
            pull = (
                jac_ref[a, part, :] * error[0]
                + jac_ref[6 + a, part, :] * error[1]
                + jac_ref[12 + a, part, :] * error[2]
            )
            for s, piece in enumerate(split3(pull)):
                planes_ref[s * 6 + a, part, :] = piece
    sums = segment_rows(
        lambda t: [planes_ref[j, pl.ds(t, 1), :] for j in range(18)],
        lambda t: pose_ref[pl.ds(t, 1), :],
        rows,
        out_rows,
    )
    for a in range(6):
        high, middle, low = (
            sums[(s * 6 + a) * out_rows : (s * 6 + a + 1) * out_rows] for s in range(3)
        )
        out_ref[a] = high + (middle + low)


def refine_kernel(edge_ref, grad_ref, inverse_ref, offset_ref, *refs):
    blocks, out_ref = refs[:-1], refs[-1]
    pose_ref = blocks[0]
    subs = len(blocks)
    rows = edge_ref.shape[0]
    count = rows * LANES
    edge = edge_ref[...]
    place = lax.rem(lax.axis_index("sub") + subs - edge // count, subs)
    tables = [
        [held[a, pl.ds(k, 1), :] for held in blocks for k in range(rows)] for a in range(6)
    ]
    far = lookup(tables, place * count + lax.rem(edge, count), rows)
    grad = [grad_ref[a] + far[a] - pose_ref[a] - offset_ref[a] for a in range(6)]
    for a in range(6):
        delta = inverse_ref[a * 6] * grad[0]
        for b in range(1, 6):
            delta = delta + inverse_ref[a * 6 + b] * grad[b]
        out_ref[a] = pose_ref[a] + delta


def finish_kernel(
    block, subs, landmark_total, recv_ref, live_ref, copies_ref, duals_ref, dual_ref, norm_ref
):
    rows = copies_ref.shape[1]
    per = LANES // block
    robots = rows * per
    me = lax.axis_index("sub")
    lane = lax.broadcasted_iota(jnp.int32, (rows, LANES), 1)
    back = [jnp.zeros((rows, LANES), jnp.float32) for _ in range(3)]
    live = live_ref[...]
    for j in range(per):
        here = (lane >= j * block) & (lane < (j + 1) * block)
        for v, (line, at) in enumerate(((0, 0), (0, block), (1, 0))):
            start = 2 * (j * subs + me) + line
            got = recv_ref[pl.ds(start, rows, 2 * subs * per), :]
            turn = (j * block - at) % LANES
            moved = pltpu.roll(got, turn, 1) if turn else got
            back[v] = jnp.where(here, moved, back[v])
    for v in range(3):
        dual_ref[v] = duals_ref[v] + (copies_ref[v] - back[v]) * live
    sums = jnp.sum(recv_ref[pl.ds(1, robots * subs, 2), :], axis=0, keepdims=True)
    norms = jnp.sqrt(sums / landmark_total)
    lane = lax.broadcasted_iota(jnp.int32, (1, LANES), 1)
    for k in range(2):
        norm_ref[k] = jnp.sum(jnp.where(lane == block + k, norms, 0.0))


VMEM = pl.BlockSpec(memory_space=pltpu.VMEM)
SMEM = pl.BlockSpec(memory_space=pltpu.SMEM)


def in_vmem(value):
    return pltpu.with_memory_space_constraint(value, pltpu.VMEM)


def call(kernel, outs, in_specs, out_specs=None, scratch=()):
    shapes = [
        jax.ShapeDtypeStruct(shape, jnp.float32) if isinstance(shape, tuple) else shape
        for shape in outs
    ]
    return pl.pallas_call(
        kernel,
        out_shape=shapes,
        in_specs=in_specs,
        out_specs=out_specs or [VMEM] * len(outs),
        scratch_shapes=list(scratch),
    )


def step(
    landmark_copies,
    dual_copies,
    visibility,
    block_counts,
    consensus_old,
    poses,
    inverse_blocks,
    jacobians,
    measurements,
    obs_pose,
    obs_slot,
    edge_to,
    edge_offset,
):
    robots = lax.axis_size("robot")
    subs = lax.axis_size("sub")
    slots = landmark_copies.shape[3]
    owned = consensus_old.shape[3]
    pose_count = poses.shape[3]
    observed = obs_slot.shape[2]
    block = slots // robots
    rows, owned_rows = slots // LANES, owned // LANES
    pose_rows, obs_rows = pose_count // LANES, observed // LANES

    copies = landmark_copies.reshape(3, rows, LANES)
    duals = dual_copies.reshape(3, rows, LANES)
    ids = visibility.reshape(rows, LANES)
    counts = block_counts.reshape(1, robots)
    old = consensus_old.reshape(3, owned_rows, LANES)
    pose_block = poses.reshape(6, pose_rows, LANES)
    inverse = inverse_blocks.reshape(36, pose_rows, LANES)
    jac = jacobians.reshape(18, obs_rows, LANES)
    measured = measurements.reshape(3, obs_rows, LANES)
    pose_ids = obs_pose.reshape(obs_rows, LANES)
    slot_ids = obs_slot.reshape(obs_rows, LANES)
    edges = edge_to.reshape(pose_rows, LANES)
    offset = edge_offset.reshape(6, pose_rows, LANES)

    held = [pose_block]
    for k in range(1, subs):
        ring = [(i, (i + k) % subs) for i in range(subs)]
        held.append(lax.ppermute(pose_block, "sub", ring))

    outgoing, live = call(
        functools.partial(pack_kernel, block),
        [
            pltpu.VMEM((robots * FIELDS, LANES), jnp.float32),
            pltpu.VMEM((rows, LANES), jnp.float32),
        ],
        [SMEM, VMEM, VMEM, VMEM],
    )(counts, copies, duals, ids)
    received = lax.all_to_all(
        outgoing.reshape(robots, FIELDS, LANES), "robot", 0, 0, tiled=True
    ).reshape(robots * FIELDS, LANES)

    (grad_obs,) = call(
        observe_kernel,
        [pltpu.VMEM((6, pose_rows, LANES), jnp.float32)],
        [VMEM] * 5,
        scratch=[pltpu.VMEM((18, obs_rows, LANES), jnp.float32)],
    )(copies, measured, jac, slot_ids, pose_ids)

    consensus, returning = call(
        functools.partial(owner_kernel, block, subs),
        [
            pltpu.VMEM((3, owned_rows, LANES), jnp.float32),
            pltpu.VMEM((robots * subs * 2, LANES), jnp.float32),
        ],
        [VMEM, VMEM],
    )(in_vmem(received), in_vmem(old))
    back = lax.all_to_all(
        returning.reshape(robots * subs, 2, LANES), ("robot", "sub"), 0, 0, tiled=True
    ).reshape(robots * subs * 2, LANES)

    (refined,) = call(
        refine_kernel, [(6, pose_rows, LANES)], [VMEM] * (4 + subs)
    )(edges, in_vmem(grad_obs), inverse, offset, *[in_vmem(value) for value in held])

    dual_new, residual_norms = call(
        functools.partial(finish_kernel, block, subs, float(owned * robots * subs)),
        [(3, rows, LANES), (2,)],
        [VMEM] * 4,
        out_specs=[VMEM, SMEM],
    )(in_vmem(back), in_vmem(live), in_vmem(copies), in_vmem(duals))
    return (
        refined.reshape(1, 1, 6, pose_count),
        consensus.reshape(1, 1, 3, owned),
        dual_new.reshape(1, 1, 3, slots),
        residual_norms,
    )


def solution(mesh):
    split4 = P("robot", "sub", None, None)
    split3d = P("robot", "sub", None)
    return jax.shard_map(
        step,
        mesh=mesh,
        in_specs=(
            split4,
            split4,
            split3d,
            split3d,
            split4,
            split4,
            split4,
            split4,
            split4,
            split3d,
            split3d,
            split3d,
            split4,
        ),
        out_specs=(split4, split4, split4, P()),
        check_vma=False,
    )
```

```python
import functools

import jax
import jax.numpy as jnp
from jax import lax
from jax.experimental import pallas as pl
from jax.experimental.pallas import tpu as pltpu
from jax.sharding import PartitionSpec as P


penalty = 2.0
LANES = 128
SUBLANES = 8
FIELDS = 8
SHIFT = LANES.bit_length() - 1
WHOLE_BYTES = 2 << 20


def split3(value):
    high = value.astype(jnp.bfloat16).astype(jnp.float32)
    rest = value - high
    middle = rest.astype(jnp.bfloat16).astype(jnp.float32)
    low = (rest - middle).astype(jnp.bfloat16).astype(jnp.float32)
    return high, middle, low


def lookup(tables, index, out_rows):
    low = index & (LANES - 1)
    high = index >> SHIFT
    results = []
    for rows in tables:
        total = None
        for k, row in enumerate(rows):
            table = jnp.broadcast_to(row, (out_rows, LANES))
            got = jnp.take_along_axis(table, low, axis=1, mode="promise_in_bounds")
            total = got if total is None else jnp.where(high == k, got, total)
        results.append(total)
    return results


def segment_rows(values, index, chunks, out_rows):
    sub = lax.broadcasted_iota(jnp.int32, (out_rows, LANES), 0)
    lane_ids = lax.broadcasted_iota(jnp.int32, (LANES, LANES), 0)
    group = min(4, chunks)
    total = None
    for start in range(0, chunks, group):
        left, right = [], []
        for t in range(start, start + group):
            ids = index(t)
            high = jnp.broadcast_to(ids >> SHIFT, (out_rows, LANES)) == sub
            low = jnp.broadcast_to(ids & (LANES - 1), (LANES, LANES)) == lane_ids
            left.append(
                jnp.concatenate(
                    [
                        jnp.where(high, jnp.broadcast_to(row, (out_rows, LANES)), 0.0)
                        for row in values(t)
                    ],
                    axis=0,
                ).astype(jnp.bfloat16)
            )
            right.append(jnp.where(low, 1.0, 0.0).astype(jnp.bfloat16))
        part = lax.dot_general(
            jnp.concatenate(left, axis=1),
            jnp.concatenate(right, axis=1),
            (((1,), (1,)), ((), ())),
            preferred_element_type=jnp.float32,
        )
        total = part if total is None else total + part
    return total


def column_of(counts_ref, first, step, rows):
    sub = lax.broadcasted_iota(jnp.int32, (rows, LANES), 0)
    result = jnp.zeros((rows, LANES), jnp.int32)
    for k in range(rows):
        result = jnp.where(sub == k, counts_ref[0, first + step * k], result)
    return result


def slot_sums(field, live, ids, out_rows):
    pieces = [split3(live * (field[v] + field[3 + v])) for v in range(3)]
    planes = [pieces[v][s] for s in range(3) for v in range(3)] + [live]
    sums = segment_rows(
        lambda t: [plane[t : t + 1] for plane in planes],
        lambda t: ids[t : t + 1],
        ids.shape[0],
        out_rows,
    )
    part = [sums[j * out_rows : (j + 1) * out_rows] for j in range(10)]
    return [part[v] + (part[3 + v] + part[6 + v]) for v in range(3)] + [part[9]]


def write_sending(pose_ref, primal, dual, out_ref):
    rows = pose_ref.shape[1]
    for a in range(6):
        out_ref[pl.ds(a * rows, rows), :] = pose_ref[a]
    primal = jnp.sum(primal, axis=0, keepdims=True)
    dual = penalty * penalty * jnp.sum(dual, axis=0, keepdims=True)
    sub = lax.broadcasted_iota(jnp.int32, (SUBLANES, LANES), 0)
    out_ref[pl.ds(6 * rows, SUBLANES), :] = jnp.where(
        sub == 0, primal, jnp.where(sub == 1, dual, 0.0)
    )


def block_rows(rows, owned_rows):
    used = FIELDS * rows + 3 * owned_rows
    return -(-used // SUBLANES) * SUBLANES


def pack_kernel(block, counts_ref, copies_ref, duals_ref, ids_ref, old_ref, out_ref, live_ref):
    rows, owned_rows = ids_ref.shape[0], old_ref.shape[1]
    height = block_rows(rows, owned_rows)
    per = LANES // block
    lane = lax.broadcasted_iota(jnp.int32, (rows, LANES), 1)
    live = jnp.zeros((rows, LANES), jnp.float32)
    for j in range(per):
        count = column_of(counts_ref, j, per, rows)
        live = jnp.where((lane >= j * block) & (lane < j * block + count), 1.0, live)
    live_ref[...] = live
    planes = [copies_ref[k] for k in range(3)] + [duals_ref[k] for k in range(3)]
    planes += [ids_ref[...].astype(jnp.float32), live] + [old_ref[k] for k in range(3)]
    used = FIELDS * rows + 3 * owned_rows
    if height > used:
        planes.append(jnp.zeros((height - used, LANES), jnp.float32))
    whole = jnp.concatenate(planes, axis=0)
    for d in range(out_ref.shape[0] // height):
        out_ref[pl.ds(d * height, height), :] = whole


def consensus_kernel(
    block, owned_rows, recv_ref, pose_ref, out_ref, back_ref, consensus_ref, backs_ref, news_ref
):
    rows = back_ref.shape[1]
    height = block_rows(rows, owned_rows)
    robots = recv_ref.shape[0] // height
    per = LANES // block
    wide = per * owned_rows
    side = lax.broadcasted_iota(jnp.int32, (robots, LANES), 1) // block * (owned_rows * LANES)
    primal = jnp.zeros((robots, LANES), jnp.float32)
    dual = jnp.zeros((wide, LANES), jnp.float32)
    for k in range(rows):
        field = [recv_ref[pl.ds(v * rows + k, robots, height), :] for v in range(FIELDS)]
        live = field[7]
        ids = field[6].astype(jnp.int32) + side
        sums = slot_sums(field, live, ids, wide)
        tables = []
        for v in range(3):
            start = FIELDS * rows + v * owned_rows
            lines = [
                recv_ref[pl.ds((k * per + j) * height + start, owned_rows), :] for j in range(per)
            ]
            old = jnp.concatenate(lines, axis=0)
            new = (old + sums[v]) / (1.0 + sums[3])
            for j in range(per):
                news_ref[v, k * per + j] = new[j * owned_rows : (j + 1) * owned_rows]
            change = new - old
            dual = dual + sums[3] * change * change
            tables.append([new[j : j + 1] for j in range(wide)])
        back = lookup(tables, ids, robots)
        for v in range(3):
            backs_ref[v, pl.ds(k * robots, robots), :] = back[v]
            differ = (field[v] - back[v]) * live
            primal = primal + differ * differ
    me = lax.axis_index("robot")
    for v in range(3):
        back_ref[v] = backs_ref[v, pl.ds(me, rows, robots), :]
        consensus_ref[v] = news_ref[v, me]
    write_sending(pose_ref, primal, dual, out_ref)


def pack_blocks_kernel(block, counts_ref, copies_ref, duals_ref, ids_ref, out_ref, live_ref):
    rows = ids_ref.shape[0]
    per = LANES // block
    lane = lax.broadcasted_iota(jnp.int32, (rows, LANES), 1)
    sources = [copies_ref[k] for k in range(3)] + [duals_ref[k] for k in range(3)]
    sources.append(ids_ref[...].astype(jnp.float32))
    mask = jnp.zeros((rows, LANES), jnp.float32)
    for j in range(per):
        for v, source in enumerate(sources):
            moved = pltpu.roll(source, LANES - j * block, 1) if j else source
            out_ref[pl.ds(j * FIELDS + v, rows, per * FIELDS), :] = moved
        count = column_of(counts_ref, j, per, rows)
        live = (lane < count).astype(jnp.float32)
        out_ref[pl.ds(j * FIELDS + 7, rows, per * FIELDS), :] = live
        here = (lane >= j * block) & (lane < j * block + count)
        mask = jnp.where(here, 1.0, mask)
    live_ref[...] = mask


def owner_kernel(block, recv_ref, old_ref, consensus_ref, out_ref):
    robots = recv_ref.shape[0] // FIELDS
    rows = old_ref.shape[1]
    field = [recv_ref[pl.ds(v, robots, FIELDS), :] for v in range(FIELDS)]
    live = field[7]
    ids = field[6].astype(jnp.int32)
    sums = slot_sums(field, live, ids, max(rows, SUBLANES))
    seen = sums[3][:rows]
    dual = jnp.zeros((rows, LANES), jnp.float32)
    tables = []
    for v in range(3):
        old = old_ref[v]
        new = (old + sums[v][:rows]) / (1.0 + seen)
        consensus_ref[v] = new
        change = new - old
        dual = dual + seen * change * change
        tables.append([new[k : k + 1] for k in range(rows)])
    back = lookup(tables, ids, robots)
    primal = jnp.zeros((robots, LANES), jnp.float32)
    for v in range(3):
        differ = (field[v] - back[v]) * live
        primal = primal + differ * differ
    primal = jnp.sum(primal, axis=(0, 1), keepdims=True)
    dual = jnp.sum(dual, axis=(0, 1), keepdims=True)
    lane = lax.broadcasted_iota(jnp.int32, (robots, LANES), 1)
    partial = jnp.where(lane == block, primal, jnp.where(lane == block + 1, dual, 0.0))
    first = jnp.where(lane < block, back[0], pltpu.roll(back[1], block, 1))
    out_ref[pl.ds(0, robots, 2), :] = first
    out_ref[pl.ds(1, robots, 2), :] = jnp.where(lane < block, back[2], partial)


def collect_kernel(block, recv_ref, pose_ref, out_ref, back_ref):
    rows = back_ref.shape[1]
    per = LANES // block
    lane = lax.broadcasted_iota(jnp.int32, (rows, LANES), 1)
    back = [jnp.zeros((rows, LANES), jnp.float32) for _ in range(3)]
    for j in range(per):
        here = (lane >= j * block) & (lane < (j + 1) * block)
        for v, (line, at) in enumerate(((0, 0), (0, block), (1, 0))):
            got = recv_ref[pl.ds(2 * j + line, rows, 2 * per), :]
            turn = (j * block - at) % LANES
            moved = pltpu.roll(got, turn, 1) if turn else got
            back[v] = jnp.where(here, moved, back[v])
    for v in range(3):
        back_ref[v] = back[v]
    partial = recv_ref[pl.ds(1, rows * per, 2), :]
    lane = lax.broadcasted_iota(jnp.int32, partial.shape, 1)
    primal = jnp.where(lane == block, partial, 0.0)
    dual = jnp.where(lane == block + 1, partial, 0.0)
    write_sending(pose_ref, primal, dual, out_ref)


def observe_kernel(
    copies_ref, measured_ref, jac_ref, slot_ref, pose_ref, duals_ref, live_ref, back_ref,
    estimate_ref, out_ref, dual_ref, consensus_ref, planes_ref,
):
    for v in range(3):
        consensus_ref[v] = estimate_ref[v]
        dual_ref[v] = duals_ref[v] + (copies_ref[v] - back_ref[v]) * live_ref[...]
    rows = slot_ref.shape[0]
    table_rows = copies_ref.shape[1]
    out_rows = out_ref.shape[1]
    for start in range(0, rows, SUBLANES):
        part = pl.ds(start, SUBLANES)
        tables = [[copies_ref[k, pl.ds(j, 1), :] for j in range(table_rows)] for k in range(3)]
        at = lookup(tables, slot_ref[part, :], SUBLANES)
        error = [measured_ref[k, part, :] - at[k] for k in range(3)]
        for a in range(6):
            pull = (
                jac_ref[a, part, :] * error[0]
                + jac_ref[6 + a, part, :] * error[1]
                + jac_ref[12 + a, part, :] * error[2]
            )
            for s, piece in enumerate(split3(pull)):
                planes_ref[s * 6 + a, part, :] = piece
    sums = segment_rows(
        lambda t: [planes_ref[j, pl.ds(t, 1), :] for j in range(18)],
        lambda t: pose_ref[pl.ds(t, 1), :],
        rows,
        out_rows,
    )
    for a in range(6):
        high, middle, low = (
            sums[(s * 6 + a) * out_rows : (s * 6 + a + 1) * out_rows] for s in range(3)
        )
        out_ref[a] = high + (middle + low)


def refine_kernel(landmark_total, edge_ref, grad_ref, inverse_ref, offset_ref, *refs):
    blocks, (out_ref, norm_ref) = refs[:-2], refs[-2:]
    subs = len(blocks)
    rows = edge_ref.shape[0]
    count = rows * LANES
    me = lax.axis_index("sub")
    edge = edge_ref[...]
    place = lax.rem(me + subs - edge // count, subs)
    tables = [
        [held[pl.ds(a * rows + k, 1), :] for held in blocks for k in range(rows)]
        for a in range(6)
    ]
    far = lookup(tables, place * count + lax.rem(edge, count), rows)
    own = [blocks[0][pl.ds(a * rows, rows), :] for a in range(6)]
    grad = [grad_ref[a] + far[a] - own[a] - offset_ref[a] for a in range(6)]
    for a in range(6):
        delta = inverse_ref[a * 6] * grad[0]
        for b in range(1, 6):
            delta = delta + inverse_ref[a * 6 + b] * grad[b]
        out_ref[a] = own[a] + delta
    total = None
    for s in range(subs):
        place = lax.rem(me + subs - s, subs)
        part = blocks[0][pl.ds(6 * rows, SUBLANES), :]
        for k in range(1, subs):
            part = jnp.where(place == k, blocks[k][pl.ds(6 * rows, SUBLANES), :], part)
        total = part if total is None else total + part
    norms = jnp.sqrt(jnp.sum(total, axis=1, keepdims=True) / landmark_total)
    for k in range(2):
        norm_ref[k] = norms[k, 0]


VMEM = pl.BlockSpec(memory_space=pltpu.VMEM)
SMEM = pl.BlockSpec(memory_space=pltpu.SMEM)


def vmem(*shape):
    return pltpu.VMEM(shape, jnp.float32)


def over_robots(value, robots):
    blocks = value.reshape(robots, value.shape[0] // robots, LANES)
    return lax.all_to_all(blocks, "robot", 0, 0, tiled=True).reshape(value.shape)


def in_vmem(value):
    return pltpu.with_memory_space_constraint(value, pltpu.VMEM)


def call(kernel, outs, in_specs, out_specs=None, scratch=()):
    shapes = [
        jax.ShapeDtypeStruct(shape, jnp.float32) if isinstance(shape, tuple) else shape
        for shape in outs
    ]
    return pl.pallas_call(
        kernel,
        out_shape=shapes,
        in_specs=in_specs,
        out_specs=out_specs or [VMEM] * len(outs),
        scratch_shapes=list(scratch),
    )


def step(
    landmark_copies,
    dual_copies,
    visibility,
    block_counts,
    consensus_old,
    poses,
    inverse_blocks,
    jacobians,
    measurements,
    obs_pose,
    obs_slot,
    edge_to,
    edge_offset,
):
    robots = lax.axis_size("robot")
    subs = lax.axis_size("sub")
    slots = landmark_copies.shape[3]
    owned = consensus_old.shape[3]
    pose_count = poses.shape[3]
    observed = obs_slot.shape[2]
    block = slots // robots
    rows, owned_rows = slots // LANES, owned // LANES
    pose_rows, obs_rows = pose_count // LANES, observed // LANES

    copies = landmark_copies.reshape(3, rows, LANES)
    duals = dual_copies.reshape(3, rows, LANES)
    ids = visibility.reshape(rows, LANES)
    counts = block_counts.reshape(1, robots)
    old = consensus_old.reshape(3, owned_rows, LANES)
    pose_block = poses.reshape(6, pose_rows, LANES)
    inverse = inverse_blocks.reshape(36, pose_rows, LANES)
    jac = jacobians.reshape(18, obs_rows, LANES)
    measured = measurements.reshape(3, obs_rows, LANES)
    pose_ids = obs_pose.reshape(obs_rows, LANES)
    slot_ids = obs_slot.reshape(obs_rows, LANES)
    edges = edge_to.reshape(pose_rows, LANES)
    offset = edge_offset.reshape(6, pose_rows, LANES)

    height = block_rows(rows, owned_rows)
    sending_rows = 6 * pose_rows + SUBLANES
    if robots * height * LANES * 4 <= WHOLE_BYTES:
        outgoing, live = call(
            functools.partial(pack_kernel, block),
            [vmem(robots * height, LANES), vmem(rows, LANES)],
            [SMEM, VMEM, VMEM, VMEM, VMEM],
        )(counts, copies, duals, ids, old)
        received = over_robots(outgoing, robots)
        sending, back, estimate = call(
            functools.partial(consensus_kernel, block, owned_rows),
            [vmem(sending_rows, LANES), vmem(3, rows, LANES), vmem(3, owned_rows, LANES)],
            [VMEM] * 2,
            scratch=[vmem(3, rows * robots, LANES), vmem(3, robots, owned_rows, LANES)],
        )(in_vmem(received), in_vmem(pose_block))
    else:
        outgoing, live = call(
            functools.partial(pack_blocks_kernel, block),
            [vmem(robots * FIELDS, LANES), vmem(rows, LANES)],
            [SMEM, VMEM, VMEM, VMEM],
        )(counts, copies, duals, ids)
        received = over_robots(outgoing, robots)
        estimate, returning = call(
            functools.partial(owner_kernel, block),
            [vmem(3, owned_rows, LANES), vmem(robots * 2, LANES)],
            [VMEM] * 2,
        )(in_vmem(received), in_vmem(old))
        sending, back = call(
            functools.partial(collect_kernel, block),
            [vmem(sending_rows, LANES), vmem(3, rows, LANES)],
            [VMEM] * 2,
        )(in_vmem(over_robots(returning, robots)), in_vmem(pose_block))

    held = [sending]
    for k in range(1, subs):
        ring = [(i, (i + k) % subs) for i in range(subs)]
        held.append(lax.ppermute(sending, "sub", ring))

    grad_obs, dual_new, consensus = call(
        observe_kernel,
        [vmem(6, pose_rows, LANES), (3, rows, LANES), (3, owned_rows, LANES)],
        [VMEM] * 9,
        scratch=[pltpu.VMEM((18, obs_rows, LANES), jnp.float32)],
    )(
        in_vmem(copies),
        in_vmem(measured),
        in_vmem(jac),
        in_vmem(slot_ids),
        in_vmem(pose_ids),
        in_vmem(duals),
        in_vmem(live),
        in_vmem(back),
        in_vmem(estimate),
    )

    refined, residual_norms = call(
        functools.partial(refine_kernel, float(owned * robots * subs)),
        [(6, pose_rows, LANES), (2,)],
        [VMEM] * (4 + subs),
        out_specs=[VMEM, SMEM],
    )(
        in_vmem(edges),
        in_vmem(grad_obs),
        in_vmem(inverse),
        in_vmem(offset),
        *[in_vmem(value) for value in held],
    )
    return (
        refined.reshape(1, 1, 6, pose_count),
        consensus.reshape(1, 1, 3, owned),
        dual_new.reshape(1, 1, 3, slots),
        residual_norms,
    )


def solution(mesh):
    split4 = P("robot", "sub", None, None)
    split3d = P("robot", "sub", None)
    return jax.shard_map(
        step,
        mesh=mesh,
        in_specs=(
            split4,
            split4,
            split3d,
            split3d,
            split4,
            split4,
            split4,
            split4,
            split4,
            split3d,
            split3d,
            split3d,
            split4,
        ),
        out_specs=(split4, split4, split4, P()),
        check_vma=False,
    )
```

```python
import functools

import jax
import jax.numpy as jnp
from jax import lax
from jax.experimental import pallas as pl
from jax.experimental.pallas import tpu as pltpu
from jax.sharding import PartitionSpec as P


penalty = 2.0
LANES = 128
SUBLANES = 8
FIELDS = 8
SHIFT = LANES.bit_length() - 1
WHOLE_BYTES = 2 << 20


def split3(value):
    high = value.astype(jnp.bfloat16).astype(jnp.float32)
    rest = value - high
    middle = rest.astype(jnp.bfloat16).astype(jnp.float32)
    low = (rest - middle).astype(jnp.bfloat16).astype(jnp.float32)
    return high, middle, low


def lookup(tables, index, out_rows):
    low = index & (LANES - 1)
    high = index >> SHIFT
    results = []
    for rows in tables:
        total = None
        for k, row in enumerate(rows):
            table = jnp.broadcast_to(row, (out_rows, LANES))
            got = jnp.take_along_axis(table, low, axis=1, mode="promise_in_bounds")
            total = got if total is None else jnp.where(high == k, got, total)
        results.append(total)
    return results


def segment_rows(values, index, chunks, out_rows):
    sub = lax.broadcasted_iota(jnp.int32, (out_rows, LANES), 0)
    lane_ids = lax.broadcasted_iota(jnp.int32, (LANES, LANES), 0)
    group = min(4, chunks)
    total = None
    for start in range(0, chunks, group):
        left, right = [], []
        for t in range(start, start + group):
            ids = index(t)
            high = jnp.broadcast_to(ids >> SHIFT, (out_rows, LANES)) == sub
            low = jnp.broadcast_to(ids & (LANES - 1), (LANES, LANES)) == lane_ids
            left.append(
                jnp.concatenate(
                    [
                        jnp.where(high, jnp.broadcast_to(row, (out_rows, LANES)), 0.0)
                        for row in values(t)
                    ],
                    axis=0,
                ).astype(jnp.bfloat16)
            )
            right.append(jnp.where(low, 1.0, 0.0).astype(jnp.bfloat16))
        part = lax.dot_general(
            jnp.concatenate(left, axis=1),
            jnp.concatenate(right, axis=1),
            (((1,), (1,)), ((), ())),
            preferred_element_type=jnp.float32,
        )
        total = part if total is None else total + part
    return total


def column_of(counts_ref, first, step, rows):
    sub = lax.broadcasted_iota(jnp.int32, (rows, LANES), 0)
    result = jnp.zeros((rows, LANES), jnp.int32)
    for k in range(rows):
        result = jnp.where(sub == k, counts_ref[0, first + step * k], result)
    return result


def slot_sums(field, live, ids, out_rows):
    pieces = [split3(live * (field[v] + field[3 + v])) for v in range(3)]
    planes = [pieces[v][s] for s in range(3) for v in range(3)] + [live]
    sums = segment_rows(
        lambda t: [plane[t : t + 1] for plane in planes],
        lambda t: ids[t : t + 1],
        ids.shape[0],
        out_rows,
    )
    part = [sums[j * out_rows : (j + 1) * out_rows] for j in range(10)]
    return [part[v] + (part[3 + v] + part[6 + v]) for v in range(3)] + [part[9]]


def write_sending(pose_ref, primal, dual, out_ref):
    rows = pose_ref.shape[1]
    for a in range(6):
        out_ref[pl.ds(a * rows, rows), :] = pose_ref[a]
    primal = jnp.sum(primal, axis=0, keepdims=True)
    dual = penalty * penalty * jnp.sum(dual, axis=0, keepdims=True)
    sub = lax.broadcasted_iota(jnp.int32, (SUBLANES, LANES), 0)
    out_ref[pl.ds(6 * rows, SUBLANES), :] = jnp.where(
        sub == 0, primal, jnp.where(sub == 1, dual, 0.0)
    )


def block_rows(rows, owned_rows):
    used = FIELDS * rows + 3 * owned_rows
    return -(-used // SUBLANES) * SUBLANES


def pack_kernel(block, counts_ref, copies_ref, duals_ref, ids_ref, old_ref, out_ref, live_ref):
    rows, owned_rows = ids_ref.shape[0], old_ref.shape[1]
    height = block_rows(rows, owned_rows)
    per = LANES // block
    lane = lax.broadcasted_iota(jnp.int32, (rows, LANES), 1)
    live = jnp.zeros((rows, LANES), jnp.float32)
    for j in range(per):
        count = column_of(counts_ref, j, per, rows)
        live = jnp.where((lane >= j * block) & (lane < j * block + count), 1.0, live)
    live_ref[...] = live
    planes = [copies_ref[k] for k in range(3)] + [duals_ref[k] for k in range(3)]
    planes += [ids_ref[...].astype(jnp.float32), live] + [old_ref[k] for k in range(3)]
    used = FIELDS * rows + 3 * owned_rows
    if height > used:
        planes.append(jnp.zeros((height - used, LANES), jnp.float32))
    whole = jnp.concatenate(planes, axis=0)
    for d in range(out_ref.shape[0] // height):
        out_ref[pl.ds(d * height, height), :] = whole


def consensus_kernel(
    block, owned_rows, order, recv_ref, pose_ref, out_ref, back_ref, consensus_ref, backs_ref, news_ref
):
    rows = back_ref.shape[1]
    height = block_rows(rows, owned_rows)
    robots = recv_ref.shape[0] // height
    per = LANES // block
    wide = per * owned_rows
    side = lax.broadcasted_iota(jnp.int32, (robots, LANES), 1) // block * (owned_rows * LANES)
    at = [order.index(r) for r in range(robots)]
    primal = jnp.zeros((robots, LANES), jnp.float32)
    dual = jnp.zeros((wide, LANES), jnp.float32)
    for k in range(rows):
        field = [recv_ref[pl.ds(v * rows + k, robots, height), :] for v in range(FIELDS)]
        live = field[7]
        ids = field[6].astype(jnp.int32) + side
        sums = slot_sums(field, live, ids, wide)
        tables = []
        for v in range(3):
            start = FIELDS * rows + v * owned_rows
            lines = [
                recv_ref[pl.ds(at[k * per + j] * height + start, owned_rows), :]
                for j in range(per)
            ]
            old = jnp.concatenate(lines, axis=0)
            new = (old + sums[v]) / (1.0 + sums[3])
            for j in range(per):
                news_ref[v, k * per + j] = new[j * owned_rows : (j + 1) * owned_rows]
            change = new - old
            dual = dual + sums[3] * change * change
            tables.append([new[j : j + 1] for j in range(wide)])
        back = lookup(tables, ids, robots)
        for v in range(3):
            backs_ref[v, pl.ds(k * robots, robots), :] = back[v]
            differ = (field[v] - back[v]) * live
            primal = primal + differ * differ
    me = lax.axis_index("robot")
    mine = sum(jnp.where(me == r, at[r], 0) for r in range(robots))
    for v in range(3):
        back_ref[v] = backs_ref[v, pl.ds(mine, rows, robots), :]
        consensus_ref[v] = news_ref[v, me]
    write_sending(pose_ref, primal, dual, out_ref)


def pack_blocks_kernel(block, counts_ref, copies_ref, duals_ref, ids_ref, out_ref, live_ref):
    rows = ids_ref.shape[0]
    per = LANES // block
    lane = lax.broadcasted_iota(jnp.int32, (rows, LANES), 1)
    sources = [copies_ref[k] for k in range(3)] + [duals_ref[k] for k in range(3)]
    sources.append(ids_ref[...].astype(jnp.float32))
    mask = jnp.zeros((rows, LANES), jnp.float32)
    for j in range(per):
        for v, source in enumerate(sources):
            moved = pltpu.roll(source, LANES - j * block, 1) if j else source
            out_ref[pl.ds(j * FIELDS + v, rows, per * FIELDS), :] = moved
        count = column_of(counts_ref, j, per, rows)
        live = (lane < count).astype(jnp.float32)
        out_ref[pl.ds(j * FIELDS + 7, rows, per * FIELDS), :] = live
        here = (lane >= j * block) & (lane < j * block + count)
        mask = jnp.where(here, 1.0, mask)
    live_ref[...] = mask


def owner_kernel(block, recv_ref, old_ref, consensus_ref, out_ref):
    robots = recv_ref.shape[0] // FIELDS
    rows = old_ref.shape[1]
    field = [recv_ref[pl.ds(v, robots, FIELDS), :] for v in range(FIELDS)]
    live = field[7]
    ids = field[6].astype(jnp.int32)
    sums = slot_sums(field, live, ids, max(rows, SUBLANES))
    seen = sums[3][:rows]
    dual = jnp.zeros((rows, LANES), jnp.float32)
    tables = []
    for v in range(3):
        old = old_ref[v]
        new = (old + sums[v][:rows]) / (1.0 + seen)
        consensus_ref[v] = new
        change = new - old
        dual = dual + seen * change * change
        tables.append([new[k : k + 1] for k in range(rows)])
    back = lookup(tables, ids, robots)
    primal = jnp.zeros((robots, LANES), jnp.float32)
    for v in range(3):
        differ = (field[v] - back[v]) * live
        primal = primal + differ * differ
    primal = jnp.sum(primal, axis=(0, 1), keepdims=True)
    dual = jnp.sum(dual, axis=(0, 1), keepdims=True)
    lane = lax.broadcasted_iota(jnp.int32, (robots, LANES), 1)
    partial = jnp.where(lane == block, primal, jnp.where(lane == block + 1, dual, 0.0))
    first = jnp.where(lane < block, back[0], pltpu.roll(back[1], block, 1))
    out_ref[pl.ds(0, robots, 2), :] = first
    out_ref[pl.ds(1, robots, 2), :] = jnp.where(lane < block, back[2], partial)


def collect_kernel(block, recv_ref, pose_ref, out_ref, back_ref):
    rows = back_ref.shape[1]
    per = LANES // block
    lane = lax.broadcasted_iota(jnp.int32, (rows, LANES), 1)
    back = [jnp.zeros((rows, LANES), jnp.float32) for _ in range(3)]
    for j in range(per):
        here = (lane >= j * block) & (lane < (j + 1) * block)
        for v, (line, at) in enumerate(((0, 0), (0, block), (1, 0))):
            got = recv_ref[pl.ds(2 * j + line, rows, 2 * per), :]
            turn = (j * block - at) % LANES
            moved = pltpu.roll(got, turn, 1) if turn else got
            back[v] = jnp.where(here, moved, back[v])
    for v in range(3):
        back_ref[v] = back[v]
    partial = recv_ref[pl.ds(1, rows * per, 2), :]
    lane = lax.broadcasted_iota(jnp.int32, partial.shape, 1)
    primal = jnp.where(lane == block, partial, 0.0)
    dual = jnp.where(lane == block + 1, partial, 0.0)
    write_sending(pose_ref, primal, dual, out_ref)


def observe_kernel(
    copies_ref, measured_ref, jac_ref, slot_ref, pose_ref, duals_ref, live_ref, back_ref,
    estimate_ref, out_ref, dual_ref, consensus_ref, planes_ref,
):
    for v in range(3):
        consensus_ref[v] = estimate_ref[v]
        dual_ref[v] = duals_ref[v] + (copies_ref[v] - back_ref[v]) * live_ref[...]
    rows = slot_ref.shape[0]
    table_rows = copies_ref.shape[1]
    out_rows = out_ref.shape[1]
    for start in range(0, rows, SUBLANES):
        part = pl.ds(start, SUBLANES)
        tables = [[copies_ref[k, pl.ds(j, 1), :] for j in range(table_rows)] for k in range(3)]
        at = lookup(tables, slot_ref[part, :], SUBLANES)
        error = [measured_ref[k, part, :] - at[k] for k in range(3)]
        for a in range(6):
            pull = (
                jac_ref[a, part, :] * error[0]
                + jac_ref[6 + a, part, :] * error[1]
                + jac_ref[12 + a, part, :] * error[2]
            )
            for s, piece in enumerate(split3(pull)):
                planes_ref[s * 6 + a, part, :] = piece
    sums = segment_rows(
        lambda t: [planes_ref[j, pl.ds(t, 1), :] for j in range(18)],
        lambda t: pose_ref[pl.ds(t, 1), :],
        rows,
        out_rows,
    )
    for a in range(6):
        high, middle, low = (
            sums[(s * 6 + a) * out_rows : (s * 6 + a + 1) * out_rows] for s in range(3)
        )
        out_ref[a] = high + (middle + low)


def refine_kernel(landmark_total, edge_ref, grad_ref, inverse_ref, offset_ref, *refs):
    blocks, (out_ref, norm_ref) = refs[:-2], refs[-2:]
    subs = len(blocks)
    rows = edge_ref.shape[0]
    count = rows * LANES
    me = lax.axis_index("sub")
    edge = edge_ref[...]
    place = lax.rem(me + subs - edge // count, subs)
    tables = [
        [held[pl.ds(a * rows + k, 1), :] for held in blocks for k in range(rows)]
        for a in range(6)
    ]
    far = lookup(tables, place * count + lax.rem(edge, count), rows)
    own = [blocks[0][pl.ds(a * rows, rows), :] for a in range(6)]
    grad = [grad_ref[a] + far[a] - own[a] - offset_ref[a] for a in range(6)]
    for a in range(6):
        delta = inverse_ref[a * 6] * grad[0]
        for b in range(1, 6):
            delta = delta + inverse_ref[a * 6 + b] * grad[b]
        out_ref[a] = own[a] + delta
    total = None
    for s in range(subs):
        place = lax.rem(me + subs - s, subs)
        part = blocks[0][pl.ds(6 * rows, SUBLANES), :]
        for k in range(1, subs):
            part = jnp.where(place == k, blocks[k][pl.ds(6 * rows, SUBLANES), :], part)
        total = part if total is None else total + part
    norms = jnp.sqrt(jnp.sum(total, axis=1, keepdims=True) / landmark_total)
    for k in range(2):
        norm_ref[k] = norms[k, 0]


VMEM = pl.BlockSpec(memory_space=pltpu.VMEM)
SMEM = pl.BlockSpec(memory_space=pltpu.SMEM)


def vmem(*shape):
    return pltpu.VMEM(shape, jnp.float32)


def meeting_order(robots):
    first = robots * 3 // 4
    if robots & (robots - 1) == 0:
        return [i ^ first for i in range(robots)]
    return [first] + [i for i in range(robots) if i != first]


def over_robots(value, robots, order=None):
    blocks = value.reshape(robots, value.shape[0] // robots, LANES)
    groups = None if order is None else [list(order)]
    moved = lax.all_to_all(blocks, "robot", 0, 0, tiled=True, axis_index_groups=groups)
    return moved.reshape(value.shape)


def in_vmem(value):
    return pltpu.with_memory_space_constraint(value, pltpu.VMEM)


def call(kernel, outs, in_specs, out_specs=None, scratch=()):
    shapes = [
        jax.ShapeDtypeStruct(shape, jnp.float32) if isinstance(shape, tuple) else shape
        for shape in outs
    ]
    return pl.pallas_call(
        kernel,
        out_shape=shapes,
        in_specs=in_specs,
        out_specs=out_specs or [VMEM] * len(outs),
        scratch_shapes=list(scratch),
    )


def step(
    landmark_copies,
    dual_copies,
    visibility,
    block_counts,
    consensus_old,
    poses,
    inverse_blocks,
    jacobians,
    measurements,
    obs_pose,
    obs_slot,
    edge_to,
    edge_offset,
):
    robots = lax.axis_size("robot")
    subs = lax.axis_size("sub")
    slots = landmark_copies.shape[3]
    owned = consensus_old.shape[3]
    pose_count = poses.shape[3]
    observed = obs_slot.shape[2]
    block = slots // robots
    rows, owned_rows = slots // LANES, owned // LANES
    pose_rows, obs_rows = pose_count // LANES, observed // LANES

    copies = landmark_copies.reshape(3, rows, LANES)
    duals = dual_copies.reshape(3, rows, LANES)
    ids = visibility.reshape(rows, LANES)
    counts = block_counts.reshape(1, robots)
    old = consensus_old.reshape(3, owned_rows, LANES)
    pose_block = poses.reshape(6, pose_rows, LANES)
    inverse = inverse_blocks.reshape(36, pose_rows, LANES)
    jac = jacobians.reshape(18, obs_rows, LANES)
    measured = measurements.reshape(3, obs_rows, LANES)
    pose_ids = obs_pose.reshape(obs_rows, LANES)
    slot_ids = obs_slot.reshape(obs_rows, LANES)
    edges = edge_to.reshape(pose_rows, LANES)
    offset = edge_offset.reshape(6, pose_rows, LANES)

    height = block_rows(rows, owned_rows)
    sending_rows = 6 * pose_rows + SUBLANES
    if robots * height * LANES * 4 <= WHOLE_BYTES:
        outgoing, live = call(
            functools.partial(pack_kernel, block),
            [vmem(robots * height, LANES), vmem(rows, LANES)],
            [SMEM, VMEM, VMEM, VMEM, VMEM],
        )(counts, copies, duals, ids, old)
        order = meeting_order(robots)
        received = over_robots(outgoing, robots, order)
        sending, back, estimate = call(
            functools.partial(consensus_kernel, block, owned_rows, order),
            [vmem(sending_rows, LANES), vmem(3, rows, LANES), vmem(3, owned_rows, LANES)],
            [VMEM] * 2,
            scratch=[vmem(3, rows * robots, LANES), vmem(3, robots, owned_rows, LANES)],
        )(in_vmem(received), in_vmem(pose_block))
    else:
        outgoing, live = call(
            functools.partial(pack_blocks_kernel, block),
            [vmem(robots * FIELDS, LANES), vmem(rows, LANES)],
            [SMEM, VMEM, VMEM, VMEM],
        )(counts, copies, duals, ids)
        received = over_robots(outgoing, robots)
        estimate, returning = call(
            functools.partial(owner_kernel, block),
            [vmem(3, owned_rows, LANES), vmem(robots * 2, LANES)],
            [VMEM] * 2,
        )(in_vmem(received), in_vmem(old))
        sending, back = call(
            functools.partial(collect_kernel, block),
            [vmem(sending_rows, LANES), vmem(3, rows, LANES)],
            [VMEM] * 2,
        )(in_vmem(over_robots(returning, robots)), in_vmem(pose_block))

    held = [sending]
    for k in range(1, subs):
        ring = [(i, (i + k) % subs) for i in range(subs)]
        held.append(lax.ppermute(sending, "sub", ring))

    grad_obs, dual_new, consensus = call(
        observe_kernel,
        [vmem(6, pose_rows, LANES), (3, rows, LANES), (3, owned_rows, LANES)],
        [VMEM] * 9,
        scratch=[pltpu.VMEM((18, obs_rows, LANES), jnp.float32)],
    )(
        in_vmem(copies),
        in_vmem(measured),
        in_vmem(jac),
        in_vmem(slot_ids),
        in_vmem(pose_ids),
        in_vmem(duals),
        in_vmem(live),
        in_vmem(back),
        in_vmem(estimate),
    )

    refined, residual_norms = call(
        functools.partial(refine_kernel, float(owned * robots * subs)),
        [(6, pose_rows, LANES), (2,)],
        [VMEM] * (4 + subs),
        out_specs=[VMEM, SMEM],
    )(
        in_vmem(edges),
        in_vmem(grad_obs),
        in_vmem(inverse),
        in_vmem(offset),
        *[in_vmem(value) for value in held],
    )
    return (
        refined.reshape(1, 1, 6, pose_count),
        consensus.reshape(1, 1, 3, owned),
        dual_new.reshape(1, 1, 3, slots),
        residual_norms,
    )


def solution(mesh):
    split4 = P("robot", "sub", None, None)
    split3d = P("robot", "sub", None)
    return jax.shard_map(
        step,
        mesh=mesh,
        in_specs=(
            split4,
            split4,
            split3d,
            split3d,
            split4,
            split4,
            split4,
            split4,
            split4,
            split3d,
            split3d,
            split3d,
            split4,
        ),
        out_specs=(split4, split4, split4, P()),
        check_vma=False,
    )
```

```python
import functools

import jax
import jax.numpy as jnp
from jax import lax
from jax.experimental import pallas as pl
from jax.experimental.pallas import tpu as pltpu
from jax.sharding import PartitionSpec as P


penalty = 2.0
LANES = 128
SUBLANES = 8
FIELDS = 8
SHIFT = LANES.bit_length() - 1
WHOLE_BYTES = 2 << 20


def split3(value):
    high = value.astype(jnp.bfloat16).astype(jnp.float32)
    rest = value - high
    middle = rest.astype(jnp.bfloat16).astype(jnp.float32)
    low = (rest - middle).astype(jnp.bfloat16).astype(jnp.float32)
    return high, middle, low


def lookup(tables, index, out_rows):
    low = index & (LANES - 1)
    high = index >> SHIFT
    results = []
    for rows in tables:
        total = None
        for k, row in enumerate(rows):
            table = jnp.broadcast_to(row, (out_rows, LANES))
            got = jnp.take_along_axis(table, low, axis=1, mode="promise_in_bounds")
            total = got if total is None else jnp.where(high == k, got, total)
        results.append(total)
    return results


def segment_rows(values, index, chunks, out_rows):
    sub = lax.broadcasted_iota(jnp.int32, (out_rows, LANES), 0)
    lane_ids = lax.broadcasted_iota(jnp.int32, (LANES, LANES), 0)
    group = min(4, chunks)
    total = None
    for start in range(0, chunks, group):
        left, right = [], []
        for t in range(start, start + group):
            ids = index(t)
            high = jnp.broadcast_to(ids >> SHIFT, (out_rows, LANES)) == sub
            low = jnp.broadcast_to(ids & (LANES - 1), (LANES, LANES)) == lane_ids
            left.append(
                jnp.concatenate(
                    [
                        jnp.where(high, jnp.broadcast_to(row, (out_rows, LANES)), 0.0)
                        for row in values(t)
                    ],
                    axis=0,
                ).astype(jnp.bfloat16)
            )
            right.append(jnp.where(low, 1.0, 0.0).astype(jnp.bfloat16))
        part = lax.dot_general(
            jnp.concatenate(left, axis=1),
            jnp.concatenate(right, axis=1),
            (((1,), (1,)), ((), ())),
            preferred_element_type=jnp.float32,
        )
        total = part if total is None else total + part
    return total


def column_of(counts_ref, first, step, rows):
    sub = lax.broadcasted_iota(jnp.int32, (rows, LANES), 0)
    result = jnp.zeros((rows, LANES), jnp.int32)
    for k in range(rows):
        result = jnp.where(sub == k, counts_ref[0, first + step * k], result)
    return result


def slot_sums(field, live, ids, out_rows):
    pieces = [split3(live * (field[v] + field[3 + v])) for v in range(3)]
    planes = [pieces[v][s] for s in range(3) for v in range(3)] + [live]
    sums = segment_rows(
        lambda t: [plane[t : t + 1] for plane in planes],
        lambda t: ids[t : t + 1],
        ids.shape[0],
        out_rows,
    )
    part = [sums[j * out_rows : (j + 1) * out_rows] for j in range(10)]
    return [part[v] + (part[3 + v] + part[6 + v]) for v in range(3)] + [part[9]]


def write_sending(pose_ref, primal, dual, out_ref):
    rows = pose_ref.shape[1]
    for a in range(6):
        out_ref[pl.ds(a * rows, rows), :] = pose_ref[a]
    primal = jnp.sum(primal, axis=0, keepdims=True)
    dual = penalty * penalty * jnp.sum(dual, axis=0, keepdims=True)
    sub = lax.broadcasted_iota(jnp.int32, (SUBLANES, LANES), 0)
    out_ref[pl.ds(6 * rows, SUBLANES), :] = jnp.where(
        sub == 0, primal, jnp.where(sub == 1, dual, 0.0)
    )


def block_rows(robots, rows, owned_rows):
    used = 7 * rows + 3 * owned_rows + 1
    while used * robots % SUBLANES:
        used += 1
    return used


def pack_kernel(block, counts_ref, copies_ref, duals_ref, ids_ref, old_ref, out_ref, live_ref):
    rows, owned_rows = ids_ref.shape[0], old_ref.shape[1]
    robots = counts_ref.shape[1]
    height = block_rows(robots, rows, owned_rows)
    per = LANES // block
    lane = lax.broadcasted_iota(jnp.int32, (rows, LANES), 1)
    live = jnp.zeros((rows, LANES), jnp.float32)
    for j in range(per):
        count = column_of(counts_ref, j, per, rows)
        live = jnp.where((lane >= j * block) & (lane < j * block + count), 1.0, live)
    live_ref[...] = live
    planes = [copies_ref[k] for k in range(3)] + [duals_ref[k] for k in range(3)]
    planes += [ids_ref[...].astype(jnp.float32)] + [old_ref[k] for k in range(3)]
    lane = lax.broadcasted_iota(jnp.int32, (1, LANES), 1)
    line = jnp.zeros((1, LANES), jnp.int32)
    for d in range(robots):
        line = jnp.where(lane == d, counts_ref[0, d], line)
    planes.append(line.astype(jnp.float32))
    for d in range(robots):
        start = d * height
        for plane in planes:
            out_ref[pl.ds(start, plane.shape[0]), :] = plane
            start += plane.shape[0]
        if start < (d + 1) * height:
            rest = (d + 1) * height - start
            out_ref[pl.ds(start, rest), :] = jnp.zeros((rest, LANES), jnp.float32)


def consensus_kernel(
    block, owned_rows, order, recv_ref, pose_ref, out_ref, back_ref, consensus_ref, backs_ref, news_ref
):
    rows = back_ref.shape[1]
    robots = len(order)
    height = block_rows(robots, rows, owned_rows)
    per = LANES // block
    wide = per * owned_rows
    lane = lax.broadcasted_iota(jnp.int32, (robots, LANES), 1)
    side = lane // block * (owned_rows * LANES)
    counts = recv_ref[pl.ds(7 * rows + 3 * owned_rows, robots, height), :].astype(jnp.int32)
    at = [order.index(r) for r in range(robots)]
    primal = jnp.zeros((robots, LANES), jnp.float32)
    dual = jnp.zeros((wide, LANES), jnp.float32)
    for k in range(rows):
        field = [recv_ref[pl.ds(v * rows + k, robots, height), :] for v in range(7)]
        live = jnp.zeros((robots, LANES), jnp.float32)
        for j in range(per):
            count = jnp.broadcast_to(counts[:, k * per + j : k * per + j + 1], live.shape)
            live = jnp.where((lane >= j * block) & (lane < j * block + count), 1.0, live)
        ids = field[6].astype(jnp.int32) + side
        sums = slot_sums(field, live, ids, wide)
        tables = []
        for v in range(3):
            start = 7 * rows + v * owned_rows
            lines = [
                recv_ref[pl.ds(at[k * per + j] * height + start, owned_rows), :]
                for j in range(per)
            ]
            old = jnp.concatenate(lines, axis=0)
            new = (old + sums[v]) / (1.0 + sums[3])
            for j in range(per):
                news_ref[v, k * per + j] = new[j * owned_rows : (j + 1) * owned_rows]
            change = new - old
            dual = dual + sums[3] * change * change
            tables.append([new[j : j + 1] for j in range(wide)])
        back = lookup(tables, ids, robots)
        for v in range(3):
            backs_ref[v, pl.ds(k * robots, robots), :] = back[v]
            differ = (field[v] - back[v]) * live
            primal = primal + differ * differ
    me = lax.axis_index("robot")
    mine = sum(jnp.where(me == r, at[r], 0) for r in range(robots))
    for v in range(3):
        back_ref[v] = backs_ref[v, pl.ds(mine, rows, robots), :]
        consensus_ref[v] = news_ref[v, me]
    write_sending(pose_ref, primal, dual, out_ref)


def pack_blocks_kernel(block, counts_ref, copies_ref, duals_ref, ids_ref, out_ref, live_ref):
    rows = ids_ref.shape[0]
    per = LANES // block
    lane = lax.broadcasted_iota(jnp.int32, (rows, LANES), 1)
    sources = [copies_ref[k] for k in range(3)] + [duals_ref[k] for k in range(3)]
    sources.append(ids_ref[...].astype(jnp.float32))
    mask = jnp.zeros((rows, LANES), jnp.float32)
    for j in range(per):
        for v, source in enumerate(sources):
            moved = pltpu.roll(source, LANES - j * block, 1) if j else source
            out_ref[pl.ds(j * FIELDS + v, rows, per * FIELDS), :] = moved
        count = column_of(counts_ref, j, per, rows)
        live = (lane < count).astype(jnp.float32)
        out_ref[pl.ds(j * FIELDS + 7, rows, per * FIELDS), :] = live
        here = (lane >= j * block) & (lane < j * block + count)
        mask = jnp.where(here, 1.0, mask)
    live_ref[...] = mask


def owner_kernel(block, recv_ref, old_ref, consensus_ref, out_ref):
    robots = recv_ref.shape[0] // FIELDS
    rows = old_ref.shape[1]
    field = [recv_ref[pl.ds(v, robots, FIELDS), :] for v in range(FIELDS)]
    live = field[7]
    ids = field[6].astype(jnp.int32)
    sums = slot_sums(field, live, ids, max(rows, SUBLANES))
    seen = sums[3][:rows]
    dual = jnp.zeros((rows, LANES), jnp.float32)
    tables = []
    for v in range(3):
        old = old_ref[v]
        new = (old + sums[v][:rows]) / (1.0 + seen)
        consensus_ref[v] = new
        change = new - old
        dual = dual + seen * change * change
        tables.append([new[k : k + 1] for k in range(rows)])
    back = lookup(tables, ids, robots)
    primal = jnp.zeros((robots, LANES), jnp.float32)
    for v in range(3):
        differ = (field[v] - back[v]) * live
        primal = primal + differ * differ
    primal = jnp.sum(primal, axis=(0, 1), keepdims=True)
    dual = jnp.sum(dual, axis=(0, 1), keepdims=True)
    lane = lax.broadcasted_iota(jnp.int32, (robots, LANES), 1)
    partial = jnp.where(lane == block, primal, jnp.where(lane == block + 1, dual, 0.0))
    first = jnp.where(lane < block, back[0], pltpu.roll(back[1], block, 1))
    out_ref[pl.ds(0, robots, 2), :] = first
    out_ref[pl.ds(1, robots, 2), :] = jnp.where(lane < block, back[2], partial)


def collect_kernel(block, recv_ref, pose_ref, out_ref, back_ref):
    rows = back_ref.shape[1]
    per = LANES // block
    lane = lax.broadcasted_iota(jnp.int32, (rows, LANES), 1)
    back = [jnp.zeros((rows, LANES), jnp.float32) for _ in range(3)]
    for j in range(per):
        here = (lane >= j * block) & (lane < (j + 1) * block)
        for v, (line, at) in enumerate(((0, 0), (0, block), (1, 0))):
            got = recv_ref[pl.ds(2 * j + line, rows, 2 * per), :]
            turn = (j * block - at) % LANES
            moved = pltpu.roll(got, turn, 1) if turn else got
            back[v] = jnp.where(here, moved, back[v])
    for v in range(3):
        back_ref[v] = back[v]
    partial = recv_ref[pl.ds(1, rows * per, 2), :]
    lane = lax.broadcasted_iota(jnp.int32, partial.shape, 1)
    primal = jnp.where(lane == block, partial, 0.0)
    dual = jnp.where(lane == block + 1, partial, 0.0)
    write_sending(pose_ref, primal, dual, out_ref)


def observe_kernel(
    copies_ref, measured_ref, jac_ref, slot_ref, pose_ref, duals_ref, live_ref, back_ref,
    estimate_ref, out_ref, dual_ref, consensus_ref, planes_ref,
):
    for v in range(3):
        consensus_ref[v] = estimate_ref[v]
        dual_ref[v] = duals_ref[v] + (copies_ref[v] - back_ref[v]) * live_ref[...]
    rows = slot_ref.shape[0]
    table_rows = copies_ref.shape[1]
    out_rows = out_ref.shape[1]
    for start in range(0, rows, SUBLANES):
        part = pl.ds(start, SUBLANES)
        tables = [[copies_ref[k, pl.ds(j, 1), :] for j in range(table_rows)] for k in range(3)]
        at = lookup(tables, slot_ref[part, :], SUBLANES)
        error = [measured_ref[k, part, :] - at[k] for k in range(3)]
        for a in range(6):
            pull = (
                jac_ref[a, part, :] * error[0]
                + jac_ref[6 + a, part, :] * error[1]
                + jac_ref[12 + a, part, :] * error[2]
            )
            for s, piece in enumerate(split3(pull)):
                planes_ref[s * 6 + a, part, :] = piece
    sums = segment_rows(
        lambda t: [planes_ref[j, pl.ds(t, 1), :] for j in range(18)],
        lambda t: pose_ref[pl.ds(t, 1), :],
        rows,
        out_rows,
    )
    for a in range(6):
        high, middle, low = (
            sums[(s * 6 + a) * out_rows : (s * 6 + a + 1) * out_rows] for s in range(3)
        )
        out_ref[a] = high + (middle + low)


def refine_kernel(landmark_total, edge_ref, grad_ref, inverse_ref, offset_ref, *refs):
    blocks, (out_ref, norm_ref) = refs[:-2], refs[-2:]
    subs = len(blocks)
    rows = edge_ref.shape[0]
    count = rows * LANES
    me = lax.axis_index("sub")
    edge = edge_ref[...]
    place = lax.rem(me + subs - edge // count, subs)
    tables = [
        [held[pl.ds(a * rows + k, 1), :] for held in blocks for k in range(rows)]
        for a in range(6)
    ]
    far = lookup(tables, place * count + lax.rem(edge, count), rows)
    own = [blocks[0][pl.ds(a * rows, rows), :] for a in range(6)]
    grad = [grad_ref[a] + far[a] - own[a] - offset_ref[a] for a in range(6)]
    for a in range(6):
        delta = inverse_ref[a * 6] * grad[0]
        for b in range(1, 6):
            delta = delta + inverse_ref[a * 6 + b] * grad[b]
        out_ref[a] = own[a] + delta
    total = None
    for s in range(subs):
        place = lax.rem(me + subs - s, subs)
        part = blocks[0][pl.ds(6 * rows, SUBLANES), :]
        for k in range(1, subs):
            part = jnp.where(place == k, blocks[k][pl.ds(6 * rows, SUBLANES), :], part)
        total = part if total is None else total + part
    norms = jnp.sqrt(jnp.sum(total, axis=1, keepdims=True) / landmark_total)
    for k in range(2):
        norm_ref[k] = norms[k, 0]


VMEM = pl.BlockSpec(memory_space=pltpu.VMEM)
SMEM = pl.BlockSpec(memory_space=pltpu.SMEM)


def vmem(*shape):
    return pltpu.VMEM(shape, jnp.float32)


TRIED_ORDERS = {8: (5, 3, 0, 7, 6, 2, 1, 4)}


def meeting_order(robots):
    first = robots * 3 // 4
    rest = [i for i in range(robots) if i != first]
    return list(TRIED_ORDERS.get(robots, [first] + rest))


def over_robots(value, robots, order=None):
    blocks = value.reshape(robots, 1, value.shape[0] // robots * LANES)
    groups = None if order is None else [list(order)]
    moved = lax.all_to_all(blocks, "robot", 0, 0, tiled=True, axis_index_groups=groups)
    return moved.reshape(value.shape)


def in_vmem(value):
    return pltpu.with_memory_space_constraint(value, pltpu.VMEM)


def call(kernel, outs, in_specs, out_specs=None, scratch=()):
    shapes = [
        jax.ShapeDtypeStruct(shape, jnp.float32) if isinstance(shape, tuple) else shape
        for shape in outs
    ]
    return pl.pallas_call(
        kernel,
        out_shape=shapes,
        in_specs=in_specs,
        out_specs=out_specs or [VMEM] * len(outs),
        scratch_shapes=list(scratch),
    )


def step(
    landmark_copies,
    dual_copies,
    visibility,
    block_counts,
    consensus_old,
    poses,
    inverse_blocks,
    jacobians,
    measurements,
    obs_pose,
    obs_slot,
    edge_to,
    edge_offset,
):
    robots = lax.axis_size("robot")
    subs = lax.axis_size("sub")
    slots = landmark_copies.shape[3]
    owned = consensus_old.shape[3]
    pose_count = poses.shape[3]
    observed = obs_slot.shape[2]
    block = slots // robots
    rows, owned_rows = slots // LANES, owned // LANES
    pose_rows, obs_rows = pose_count // LANES, observed // LANES

    copies = landmark_copies.reshape(3, rows, LANES)
    duals = dual_copies.reshape(3, rows, LANES)
    ids = visibility.reshape(rows, LANES)
    counts = block_counts.reshape(1, robots)
    old = consensus_old.reshape(3, owned_rows, LANES)
    pose_block = poses.reshape(6, pose_rows, LANES)
    inverse = inverse_blocks.reshape(36, pose_rows, LANES)
    jac = jacobians.reshape(18, obs_rows, LANES)
    measured = measurements.reshape(3, obs_rows, LANES)
    pose_ids = obs_pose.reshape(obs_rows, LANES)
    slot_ids = obs_slot.reshape(obs_rows, LANES)
    edges = edge_to.reshape(pose_rows, LANES)
    offset = edge_offset.reshape(6, pose_rows, LANES)

    height = block_rows(robots, rows, owned_rows)
    sending_rows = 6 * pose_rows + SUBLANES
    if robots * height * LANES * 4 <= WHOLE_BYTES:
        outgoing, live = call(
            functools.partial(pack_kernel, block),
            [vmem(robots * height, LANES), vmem(rows, LANES)],
            [SMEM, VMEM, VMEM, VMEM, VMEM],
        )(counts, copies, duals, ids, old)
        order = meeting_order(robots)
        received = over_robots(outgoing, robots, order)
        sending, back, estimate = call(
            functools.partial(consensus_kernel, block, owned_rows, order),
            [vmem(sending_rows, LANES), vmem(3, rows, LANES), vmem(3, owned_rows, LANES)],
            [VMEM] * 2,
            scratch=[vmem(3, rows * robots, LANES), vmem(3, robots, owned_rows, LANES)],
        )(in_vmem(received), in_vmem(pose_block))
    else:
        outgoing, live = call(
            functools.partial(pack_blocks_kernel, block),
            [vmem(robots * FIELDS, LANES), vmem(rows, LANES)],
            [SMEM, VMEM, VMEM, VMEM],
        )(counts, copies, duals, ids)
        received = over_robots(outgoing, robots)
        estimate, returning = call(
            functools.partial(owner_kernel, block),
            [vmem(3, owned_rows, LANES), vmem(robots * 2, LANES)],
            [VMEM] * 2,
        )(in_vmem(received), in_vmem(old))
        sending, back = call(
            functools.partial(collect_kernel, block),
            [vmem(sending_rows, LANES), vmem(3, rows, LANES)],
            [VMEM] * 2,
        )(in_vmem(over_robots(returning, robots)), in_vmem(pose_block))

    held = [sending]
    for k in range(1, subs):
        ring = [(i, (i + k) % subs) for i in range(subs)]
        held.append(lax.ppermute(sending, "sub", ring))

    grad_obs, dual_new, consensus = call(
        observe_kernel,
        [vmem(6, pose_rows, LANES), (3, rows, LANES), (3, owned_rows, LANES)],
        [VMEM] * 9,
        scratch=[pltpu.VMEM((18, obs_rows, LANES), jnp.float32)],
    )(
        in_vmem(copies),
        in_vmem(measured),
        in_vmem(jac),
        in_vmem(slot_ids),
        in_vmem(pose_ids),
        in_vmem(duals),
        in_vmem(live),
        in_vmem(back),
        in_vmem(estimate),
    )

    refined, residual_norms = call(
        functools.partial(refine_kernel, float(owned * robots * subs)),
        [(6, pose_rows, LANES), (2,)],
        [VMEM] * (4 + subs),
        out_specs=[VMEM, SMEM],
    )(
        in_vmem(edges),
        in_vmem(grad_obs),
        in_vmem(inverse),
        in_vmem(offset),
        *[in_vmem(value) for value in held],
    )
    return (
        refined.reshape(1, 1, 6, pose_count),
        consensus.reshape(1, 1, 3, owned),
        dual_new.reshape(1, 1, 3, slots),
        residual_norms,
    )


def solution(mesh):
    split4 = P("robot", "sub", None, None)
    split3d = P("robot", "sub", None)
    return jax.shard_map(
        step,
        mesh=mesh,
        in_specs=(
            split4,
            split4,
            split3d,
            split3d,
            split4,
            split4,
            split4,
            split4,
            split4,
            split3d,
            split3d,
            split3d,
            split4,
        ),
        out_specs=(split4, split4, split4, P()),
        check_vma=False,
    )
```

```python
import functools

import jax
import jax.numpy as jnp
from jax import lax
from jax.experimental import pallas as pl
from jax.experimental.pallas import tpu as pltpu
from jax.sharding import PartitionSpec as P


penalty = 2.0
LANES = 128
SUBLANES = 8
FIELDS = 8
SHIFT = LANES.bit_length() - 1
WHOLE_BYTES = 2 << 20


def split3(value):
    high = value.astype(jnp.bfloat16).astype(jnp.float32)
    rest = value - high
    middle = rest.astype(jnp.bfloat16).astype(jnp.float32)
    low = (rest - middle).astype(jnp.bfloat16).astype(jnp.float32)
    return high, middle, low


def lookup(tables, index, out_rows):
    low = index & (LANES - 1)
    high = index >> SHIFT
    results = []
    for rows in tables:
        total = None
        for k, row in enumerate(rows):
            table = jnp.broadcast_to(row, (out_rows, LANES))
            got = jnp.take_along_axis(table, low, axis=1, mode="promise_in_bounds")
            total = got if total is None else jnp.where(high == k, got, total)
        results.append(total)
    return results


def segment_rows(values, index, chunks, out_rows):
    sub = lax.broadcasted_iota(jnp.int32, (out_rows, LANES), 0)
    lane_ids = lax.broadcasted_iota(jnp.int32, (LANES, LANES), 0)
    group = min(4, chunks)
    total = None
    for start in range(0, chunks, group):
        left, right = [], []
        for t in range(start, start + group):
            ids = index(t)
            high = jnp.broadcast_to(ids >> SHIFT, (out_rows, LANES)) == sub
            low = jnp.broadcast_to(ids & (LANES - 1), (LANES, LANES)) == lane_ids
            left.append(
                jnp.concatenate(
                    [
                        jnp.where(high, jnp.broadcast_to(row, (out_rows, LANES)), 0.0)
                        for row in values(t)
                    ],
                    axis=0,
                ).astype(jnp.bfloat16)
            )
            right.append(jnp.where(low, 1.0, 0.0).astype(jnp.bfloat16))
        part = lax.dot_general(
            jnp.concatenate(left, axis=1),
            jnp.concatenate(right, axis=1),
            (((1,), (1,)), ((), ())),
            preferred_element_type=jnp.float32,
        )
        total = part if total is None else total + part
    return total


def column_of(counts_ref, first, step, rows):
    sub = lax.broadcasted_iota(jnp.int32, (rows, LANES), 0)
    result = jnp.zeros((rows, LANES), jnp.int32)
    for k in range(rows):
        result = jnp.where(sub == k, counts_ref[0, first + step * k], result)
    return result


def slot_sums(field, live, ids, out_rows):
    pieces = [split3(live * (field[v] + field[3 + v])) for v in range(3)]
    planes = [pieces[v][s] for s in range(3) for v in range(3)] + [live]
    sums = segment_rows(
        lambda t: [plane[t : t + 1] for plane in planes],
        lambda t: ids[t : t + 1],
        ids.shape[0],
        out_rows,
    )
    part = [sums[j * out_rows : (j + 1) * out_rows] for j in range(10)]
    return [part[v] + (part[3 + v] + part[6 + v]) for v in range(3)] + [part[9]]


def write_sending(pose_ref, primal, dual, out_ref):
    rows = pose_ref.shape[1]
    for a in range(6):
        out_ref[pl.ds(a * rows, rows), :] = pose_ref[a]
    primal = jnp.sum(primal, axis=0, keepdims=True)
    dual = penalty * penalty * jnp.sum(dual, axis=0, keepdims=True)
    sub = lax.broadcasted_iota(jnp.int32, (SUBLANES, LANES), 0)
    out_ref[pl.ds(6 * rows, SUBLANES), :] = jnp.where(
        sub == 0, primal, jnp.where(sub == 1, dual, 0.0)
    )


def block_rows(robots, rows, owned_rows):
    used = 7 * rows + 3 * owned_rows + 1
    while used * robots % SUBLANES:
        used += 1
    return used


def pack_kernel(block, counts_ref, copies_ref, duals_ref, ids_ref, old_ref, edge_ref, out_ref, live_ref, c_ref, d_ref, e_ref):
    rows, owned_rows = ids_ref.shape[0], old_ref.shape[1]
    robots = counts_ref.shape[1]
    height = block_rows(robots, rows, owned_rows)
    per = LANES // block
    lane = lax.broadcasted_iota(jnp.int32, (rows, LANES), 1)
    live = jnp.zeros((rows, LANES), jnp.float32)
    for j in range(per):
        count = column_of(counts_ref, j, per, rows)
        live = jnp.where((lane >= j * block) & (lane < j * block + count), 1.0, live)
    live_ref[...] = live
    c_ref[...] = copies_ref[...]
    d_ref[...] = duals_ref[...]
    e_ref[...] = edge_ref[...]
    planes = [copies_ref[k] for k in range(3)] + [duals_ref[k] for k in range(3)]
    planes += [ids_ref[...].astype(jnp.float32)] + [old_ref[k] for k in range(3)]
    lane = lax.broadcasted_iota(jnp.int32, (1, LANES), 1)
    line = jnp.zeros((1, LANES), jnp.int32)
    for d in range(robots):
        line = jnp.where(lane == d, counts_ref[0, d], line)
    planes.append(line.astype(jnp.float32))
    for d in range(robots):
        start = d * height
        for plane in planes:
            out_ref[pl.ds(start, plane.shape[0]), :] = plane
            start += plane.shape[0]
        if start < (d + 1) * height:
            rest = (d + 1) * height - start
            out_ref[pl.ds(start, rest), :] = jnp.zeros((rest, LANES), jnp.float32)


def consensus_kernel(
    block, owned_rows, order, recv_ref, pose_ref, out_ref, back_ref, consensus_ref, backs_ref, news_ref
):
    rows = back_ref.shape[1]
    robots = len(order)
    height = block_rows(robots, rows, owned_rows)
    per = LANES // block
    wide = per * owned_rows
    lane = lax.broadcasted_iota(jnp.int32, (robots, LANES), 1)
    side = lane // block * (owned_rows * LANES)
    counts = recv_ref[pl.ds(7 * rows + 3 * owned_rows, robots, height), :].astype(jnp.int32)
    at = [order.index(r) for r in range(robots)]
    primal = jnp.zeros((robots, LANES), jnp.float32)
    dual = jnp.zeros((wide, LANES), jnp.float32)
    for k in range(rows):
        field = [recv_ref[pl.ds(v * rows + k, robots, height), :] for v in range(7)]
        live = jnp.zeros((robots, LANES), jnp.float32)
        for j in range(per):
            count = jnp.broadcast_to(counts[:, k * per + j : k * per + j + 1], live.shape)
            live = jnp.where((lane >= j * block) & (lane < j * block + count), 1.0, live)
        ids = field[6].astype(jnp.int32) + side
        sums = slot_sums(field, live, ids, wide)
        tables = []
        for v in range(3):
            start = 7 * rows + v * owned_rows
            lines = [
                recv_ref[pl.ds(at[k * per + j] * height + start, owned_rows), :]
                for j in range(per)
            ]
            old = jnp.concatenate(lines, axis=0)
            new = (old + sums[v]) / (1.0 + sums[3])
            for j in range(per):
                news_ref[v, k * per + j] = new[j * owned_rows : (j + 1) * owned_rows]
            change = new - old
            dual = dual + sums[3] * change * change
            tables.append([new[j : j + 1] for j in range(wide)])
        back = lookup(tables, ids, robots)
        for v in range(3):
            backs_ref[v, pl.ds(k * robots, robots), :] = back[v]
            differ = (field[v] - back[v]) * live
            primal = primal + differ * differ
    me = lax.axis_index("robot")
    mine = sum(jnp.where(me == r, at[r], 0) for r in range(robots))
    for v in range(3):
        back_ref[v] = backs_ref[v, pl.ds(mine, rows, robots), :]
        consensus_ref[v] = news_ref[v, me]
    write_sending(pose_ref, primal, dual, out_ref)


def pack_blocks_kernel(block, counts_ref, copies_ref, duals_ref, ids_ref, out_ref, live_ref):
    rows = ids_ref.shape[0]
    per = LANES // block
    lane = lax.broadcasted_iota(jnp.int32, (rows, LANES), 1)
    sources = [copies_ref[k] for k in range(3)] + [duals_ref[k] for k in range(3)]
    sources.append(ids_ref[...].astype(jnp.float32))
    mask = jnp.zeros((rows, LANES), jnp.float32)
    for j in range(per):
        for v, source in enumerate(sources):
            moved = pltpu.roll(source, LANES - j * block, 1) if j else source
            out_ref[pl.ds(j * FIELDS + v, rows, per * FIELDS), :] = moved
        count = column_of(counts_ref, j, per, rows)
        live = (lane < count).astype(jnp.float32)
        out_ref[pl.ds(j * FIELDS + 7, rows, per * FIELDS), :] = live
        here = (lane >= j * block) & (lane < j * block + count)
        mask = jnp.where(here, 1.0, mask)
    live_ref[...] = mask


def owner_kernel(block, recv_ref, old_ref, consensus_ref, out_ref):
    robots = recv_ref.shape[0] // FIELDS
    rows = old_ref.shape[1]
    field = [recv_ref[pl.ds(v, robots, FIELDS), :] for v in range(FIELDS)]
    live = field[7]
    ids = field[6].astype(jnp.int32)
    sums = slot_sums(field, live, ids, max(rows, SUBLANES))
    seen = sums[3][:rows]
    dual = jnp.zeros((rows, LANES), jnp.float32)
    tables = []
    for v in range(3):
        old = old_ref[v]
        new = (old + sums[v][:rows]) / (1.0 + seen)
        consensus_ref[v] = new
        change = new - old
        dual = dual + seen * change * change
        tables.append([new[k : k + 1] for k in range(rows)])
    back = lookup(tables, ids, robots)
    primal = jnp.zeros((robots, LANES), jnp.float32)
    for v in range(3):
        differ = (field[v] - back[v]) * live
        primal = primal + differ * differ
    primal = jnp.sum(primal, axis=(0, 1), keepdims=True)
    dual = jnp.sum(dual, axis=(0, 1), keepdims=True)
    lane = lax.broadcasted_iota(jnp.int32, (robots, LANES), 1)
    partial = jnp.where(lane == block, primal, jnp.where(lane == block + 1, dual, 0.0))
    first = jnp.where(lane < block, back[0], pltpu.roll(back[1], block, 1))
    out_ref[pl.ds(0, robots, 2), :] = first
    out_ref[pl.ds(1, robots, 2), :] = jnp.where(lane < block, back[2], partial)


def collect_kernel(block, recv_ref, pose_ref, out_ref, back_ref):
    rows = back_ref.shape[1]
    per = LANES // block
    lane = lax.broadcasted_iota(jnp.int32, (rows, LANES), 1)
    back = [jnp.zeros((rows, LANES), jnp.float32) for _ in range(3)]
    for j in range(per):
        here = (lane >= j * block) & (lane < (j + 1) * block)
        for v, (line, at) in enumerate(((0, 0), (0, block), (1, 0))):
            got = recv_ref[pl.ds(2 * j + line, rows, 2 * per), :]
            turn = (j * block - at) % LANES
            moved = pltpu.roll(got, turn, 1) if turn else got
            back[v] = jnp.where(here, moved, back[v])
    for v in range(3):
        back_ref[v] = back[v]
    partial = recv_ref[pl.ds(1, rows * per, 2), :]
    lane = lax.broadcasted_iota(jnp.int32, partial.shape, 1)
    primal = jnp.where(lane == block, partial, 0.0)
    dual = jnp.where(lane == block + 1, partial, 0.0)
    write_sending(pose_ref, primal, dual, out_ref)


def observe_kernel(
    copies_ref, measured_ref, jac_ref, slot_ref, pose_ref, duals_ref, live_ref, back_ref,
    estimate_ref, out_ref, dual_ref, consensus_ref, planes_ref,
):
    for v in range(3):
        consensus_ref[v] = estimate_ref[v]
        dual_ref[v] = duals_ref[v] + (copies_ref[v] - back_ref[v]) * live_ref[...]
    rows = slot_ref.shape[0]
    table_rows = copies_ref.shape[1]
    out_rows = out_ref.shape[1]
    for start in range(0, rows, SUBLANES):
        part = pl.ds(start, SUBLANES)
        tables = [[copies_ref[k, pl.ds(j, 1), :] for j in range(table_rows)] for k in range(3)]
        at = lookup(tables, slot_ref[part, :], SUBLANES)
        error = [measured_ref[k, part, :] - at[k] for k in range(3)]
        for a in range(6):
            pull = (
                jac_ref[a, part, :] * error[0]
                + jac_ref[6 + a, part, :] * error[1]
                + jac_ref[12 + a, part, :] * error[2]
            )
            for s, piece in enumerate(split3(pull)):
                planes_ref[s * 6 + a, part, :] = piece
    sums = segment_rows(
        lambda t: [planes_ref[j, pl.ds(t, 1), :] for j in range(18)],
        lambda t: pose_ref[pl.ds(t, 1), :],
        rows,
        out_rows,
    )
    for a in range(6):
        high, middle, low = (
            sums[(s * 6 + a) * out_rows : (s * 6 + a + 1) * out_rows] for s in range(3)
        )
        out_ref[a] = high + (middle + low)


def refine_kernel(landmark_total, edge_ref, grad_ref, inverse_ref, offset_ref, *refs):
    blocks, (out_ref, norm_ref) = refs[:-2], refs[-2:]
    subs = len(blocks)
    rows = edge_ref.shape[0]
    count = rows * LANES
    me = lax.axis_index("sub")
    edge = edge_ref[...]
    place = lax.bitwise_xor(edge // count, me)
    tables = [
        [held[pl.ds(a * rows + k, 1), :] for held in blocks for k in range(rows)]
        for a in range(6)
    ]
    far = lookup(tables, place * count + lax.rem(edge, count), rows)
    own = [blocks[0][pl.ds(a * rows, rows), :] for a in range(6)]
    grad = [grad_ref[a] + far[a] - own[a] - offset_ref[a] for a in range(6)]
    for a in range(6):
        delta = inverse_ref[a * 6] * grad[0]
        for b in range(1, 6):
            delta = delta + inverse_ref[a * 6 + b] * grad[b]
        out_ref[a] = own[a] + delta
    total = None
    for s in range(subs):
        place = lax.bitwise_xor(me, jnp.int32(s))
        part = blocks[0][pl.ds(6 * rows, SUBLANES), :]
        for k in range(1, subs):
            part = jnp.where(place == k, blocks[k][pl.ds(6 * rows, SUBLANES), :], part)
        total = part if total is None else total + part
    norms = jnp.sqrt(jnp.sum(total, axis=1, keepdims=True) / landmark_total)
    for k in range(2):
        norm_ref[k] = norms[k, 0]


VMEM = pl.BlockSpec(memory_space=pltpu.VMEM)
SMEM = pl.BlockSpec(memory_space=pltpu.SMEM)


def vmem(*shape):
    return pltpu.VMEM(shape, jnp.float32)


TRIED_ORDERS = {8: (5, 3, 0, 7, 6, 2, 1, 4)}


def meeting_order(robots):
    first = robots * 3 // 4
    rest = [i for i in range(robots) if i != first]
    return list(TRIED_ORDERS.get(robots, [first] + rest))


def over_robots(value, robots, order=None):
    blocks = value.reshape(robots, 1, value.shape[0] // robots * LANES)
    groups = None if order is None else [list(order)]
    moved = lax.all_to_all(blocks, "robot", 0, 0, tiled=True, axis_index_groups=groups)
    return moved.reshape(value.shape)


def in_vmem(value):
    return pltpu.with_memory_space_constraint(value, pltpu.VMEM)


def call(kernel, outs, in_specs, out_specs=None, scratch=()):
    shapes = [
        jax.ShapeDtypeStruct(shape, jnp.float32) if isinstance(shape, tuple) else shape
        for shape in outs
    ]
    return pl.pallas_call(
        kernel,
        out_shape=shapes,
        in_specs=in_specs,
        out_specs=out_specs or [VMEM] * len(outs),
        scratch_shapes=list(scratch),
    )


def step(
    landmark_copies,
    dual_copies,
    visibility,
    block_counts,
    consensus_old,
    poses,
    inverse_blocks,
    jacobians,
    measurements,
    obs_pose,
    obs_slot,
    edge_to,
    edge_offset,
):
    robots = lax.axis_size("robot")
    subs = lax.axis_size("sub")
    slots = landmark_copies.shape[3]
    owned = consensus_old.shape[3]
    pose_count = poses.shape[3]
    observed = obs_slot.shape[2]
    block = slots // robots
    rows, owned_rows = slots // LANES, owned // LANES
    pose_rows, obs_rows = pose_count // LANES, observed // LANES

    copies = landmark_copies.reshape(3, rows, LANES)
    duals = dual_copies.reshape(3, rows, LANES)
    ids = visibility.reshape(rows, LANES)
    counts = block_counts.reshape(1, robots)
    old = consensus_old.reshape(3, owned_rows, LANES)
    pose_block = poses.reshape(6, pose_rows, LANES)
    inverse = inverse_blocks.reshape(36, pose_rows, LANES)
    jac = jacobians.reshape(18, obs_rows, LANES)
    measured = measurements.reshape(3, obs_rows, LANES)
    pose_ids = obs_pose.reshape(obs_rows, LANES)
    slot_ids = obs_slot.reshape(obs_rows, LANES)
    edges = edge_to.reshape(pose_rows, LANES)
    offset = edge_offset.reshape(6, pose_rows, LANES)

    height = block_rows(robots, rows, owned_rows)
    sending_rows = 6 * pose_rows + SUBLANES
    if robots * height * LANES * 4 <= WHOLE_BYTES:
        outgoing, live, copies, duals, edges = call(
            functools.partial(pack_kernel, block),
            [vmem(robots * height, LANES), vmem(rows, LANES)]
            + [vmem(3, rows, LANES)] * 2
            + [pltpu.VMEM((pose_rows, LANES), jnp.int32)],
            [SMEM] + [VMEM] * 5,
        )(counts, copies, duals, ids, old, edges)
        order = meeting_order(robots)
        received = over_robots(outgoing, robots, order)
        sending, back, estimate = call(
            functools.partial(consensus_kernel, block, owned_rows, order),
            [vmem(sending_rows, LANES), vmem(3, rows, LANES), vmem(3, owned_rows, LANES)],
            [VMEM] * 2,
            scratch=[vmem(3, rows * robots, LANES), vmem(3, robots, owned_rows, LANES)],
        )(in_vmem(received), in_vmem(pose_block))
    else:
        outgoing, live = call(
            functools.partial(pack_blocks_kernel, block),
            [vmem(robots * FIELDS, LANES), vmem(rows, LANES)],
            [SMEM, VMEM, VMEM, VMEM],
        )(counts, copies, duals, ids)
        received = over_robots(outgoing, robots)
        estimate, returning = call(
            functools.partial(owner_kernel, block),
            [vmem(3, owned_rows, LANES), vmem(robots * 2, LANES)],
            [VMEM] * 2,
        )(in_vmem(received), in_vmem(old))
        sending, back = call(
            functools.partial(collect_kernel, block),
            [vmem(sending_rows, LANES), vmem(3, rows, LANES)],
            [VMEM] * 2,
        )(in_vmem(over_robots(returning, robots)), in_vmem(pose_block))

    held = [sending]
    for k in range(1, subs):
        ring = [(i, i ^ k) for i in range(subs)]
        held.append(lax.ppermute(sending, "sub", ring))

    grad_obs, dual_new, consensus = call(
        observe_kernel,
        [vmem(6, pose_rows, LANES), (3, rows, LANES), (3, owned_rows, LANES)],
        [VMEM] * 9,
        scratch=[pltpu.VMEM((18, obs_rows, LANES), jnp.float32)],
    )(
        in_vmem(copies),
        in_vmem(measured),
        in_vmem(jac),
        in_vmem(slot_ids),
        in_vmem(pose_ids),
        in_vmem(duals),
        in_vmem(live),
        in_vmem(back),
        in_vmem(estimate),
    )

    refined, residual_norms = call(
        functools.partial(refine_kernel, float(owned * robots * subs)),
        [(6, pose_rows, LANES), (2,)],
        [VMEM] * (4 + subs),
        out_specs=[VMEM, SMEM],
    )(
        in_vmem(edges),
        in_vmem(grad_obs),
        in_vmem(inverse),
        in_vmem(offset),
        *[in_vmem(value) for value in held],
    )
    return (
        refined.reshape(1, 1, 6, pose_count),
        consensus.reshape(1, 1, 3, owned),
        dual_new.reshape(1, 1, 3, slots),
        residual_norms,
    )


def solution(mesh):
    split4 = P("robot", "sub", None, None)
    split3d = P("robot", "sub", None)
    return jax.shard_map(
        step,
        mesh=mesh,
        in_specs=(
            split4,
            split4,
            split3d,
            split3d,
            split4,
            split4,
            split4,
            split4,
            split4,
            split3d,
            split3d,
            split3d,
            split4,
        ),
        out_specs=(split4, split4, split4, P()),
        check_vma=False,
    )
```

```python
import functools

import jax
import jax.numpy as jnp
from jax import lax
from jax.experimental import pallas as pl
from jax.experimental.pallas import tpu as pltpu
from jax.sharding import PartitionSpec as P


penalty = 2.0
LANES = 128
SUBLANES = 8
FIELDS = 8
SHIFT = LANES.bit_length() - 1
WHOLE_BYTES = 2 << 20


def split3(value):
    high = value.astype(jnp.bfloat16).astype(jnp.float32)
    rest = value - high
    middle = rest.astype(jnp.bfloat16).astype(jnp.float32)
    low = (rest - middle).astype(jnp.bfloat16).astype(jnp.float32)
    return high, middle, low


def lookup(tables, index, out_rows):
    low = index & (LANES - 1)
    high = index >> SHIFT
    results = []
    for rows in tables:
        total = None
        for k, row in enumerate(rows):
            table = jnp.broadcast_to(row, (out_rows, LANES))
            got = jnp.take_along_axis(table, low, axis=1, mode="promise_in_bounds")
            total = got if total is None else jnp.where(high == k, got, total)
        results.append(total)
    return results


def segment_rows(values, index, chunks, out_rows):
    sub = lax.broadcasted_iota(jnp.int32, (out_rows, LANES), 0)
    lane_ids = lax.broadcasted_iota(jnp.int32, (LANES, LANES), 0)
    group = min(4, chunks)
    total = None
    for start in range(0, chunks, group):
        left, right = [], []
        for t in range(start, start + group):
            ids = index(t)
            high = jnp.broadcast_to(ids >> SHIFT, (out_rows, LANES)) == sub
            low = jnp.broadcast_to(ids & (LANES - 1), (LANES, LANES)) == lane_ids
            left.append(
                jnp.concatenate(
                    [
                        jnp.where(high, jnp.broadcast_to(row, (out_rows, LANES)), 0.0)
                        for row in values(t)
                    ],
                    axis=0,
                ).astype(jnp.bfloat16)
            )
            right.append(jnp.where(low, 1.0, 0.0).astype(jnp.bfloat16))
        part = lax.dot_general(
            jnp.concatenate(left, axis=1),
            jnp.concatenate(right, axis=1),
            (((1,), (1,)), ((), ())),
            preferred_element_type=jnp.float32,
        )
        total = part if total is None else total + part
    return total


def column_of(counts_ref, first, step, rows):
    sub = lax.broadcasted_iota(jnp.int32, (rows, LANES), 0)
    result = jnp.zeros((rows, LANES), jnp.int32)
    for k in range(rows):
        result = jnp.where(sub == k, counts_ref[0, first + step * k], result)
    return result


def slot_sums(field, live, ids, out_rows):
    pieces = [split3(live * (field[v] + field[3 + v])) for v in range(3)]
    planes = [pieces[v][s] for s in range(3) for v in range(3)] + [live]
    sums = segment_rows(
        lambda t: [plane[t : t + 1] for plane in planes],
        lambda t: ids[t : t + 1],
        ids.shape[0],
        out_rows,
    )
    part = [sums[j * out_rows : (j + 1) * out_rows] for j in range(10)]
    return [part[v] + (part[3 + v] + part[6 + v]) for v in range(3)] + [part[9]]


def write_sending(pose_ref, primal, dual, out_ref):
    rows = pose_ref.shape[1]
    for a in range(6):
        out_ref[pl.ds(a * rows, rows), :] = pose_ref[a]
    primal = jnp.sum(primal, axis=0, keepdims=True)
    dual = penalty * penalty * jnp.sum(dual, axis=0, keepdims=True)
    sub = lax.broadcasted_iota(jnp.int32, (SUBLANES, LANES), 0)
    out_ref[pl.ds(6 * rows, SUBLANES), :] = jnp.where(
        sub == 0, primal, jnp.where(sub == 1, dual, 0.0)
    )


def block_rows(robots, rows, owned_rows):
    used = 7 * rows + 3 * owned_rows + 1
    while used * robots % SUBLANES:
        used += 1
    return used


def pack_kernel(block, counts_ref, copies_ref, duals_ref, ids_ref, old_ref, edge_ref, out_ref, live_ref, c_ref, d_ref, e_ref):
    rows, owned_rows = ids_ref.shape[0], old_ref.shape[1]
    robots = counts_ref.shape[1]
    height = block_rows(robots, rows, owned_rows)
    per = LANES // block
    lane = lax.broadcasted_iota(jnp.int32, (rows, LANES), 1)
    live = jnp.zeros((rows, LANES), jnp.float32)
    for j in range(per):
        count = column_of(counts_ref, j, per, rows)
        live = jnp.where((lane >= j * block) & (lane < j * block + count), 1.0, live)
    live_ref[...] = live
    c_ref[...] = copies_ref[...]
    d_ref[...] = duals_ref[...]
    e_ref[...] = edge_ref[...]
    planes = [copies_ref[k] for k in range(3)] + [duals_ref[k] for k in range(3)]
    planes += [ids_ref[...].astype(jnp.float32)] + [old_ref[k] for k in range(3)]
    lane = lax.broadcasted_iota(jnp.int32, (1, LANES), 1)
    line = jnp.zeros((1, LANES), jnp.int32)
    for d in range(robots):
        line = jnp.where(lane == d, counts_ref[0, d], line)
    planes.append(line.astype(jnp.float32))
    for d in range(robots):
        start = d * height
        for plane in planes:
            out_ref[pl.ds(start, plane.shape[0]), :] = plane
            start += plane.shape[0]
        if start < (d + 1) * height:
            rest = (d + 1) * height - start
            out_ref[pl.ds(start, rest), :] = jnp.zeros((rest, LANES), jnp.float32)


def consensus_kernel(
    block, owned_rows, order, recv_ref, pose_ref, out_ref, back_ref, consensus_ref, backs_ref, news_ref
):
    rows = back_ref.shape[1]
    robots = len(order)
    height = block_rows(robots, rows, owned_rows)
    per = LANES // block
    wide = per * owned_rows
    lane = lax.broadcasted_iota(jnp.int32, (robots, LANES), 1)
    side = lane // block * (owned_rows * LANES)
    counts = recv_ref[pl.ds(7 * rows + 3 * owned_rows, robots, height), :].astype(jnp.int32)
    at = [order.index(r) for r in range(robots)]
    primal = jnp.zeros((robots, LANES), jnp.float32)
    dual = jnp.zeros((wide, LANES), jnp.float32)
    for k in range(rows):
        field = [recv_ref[pl.ds(v * rows + k, robots, height), :] for v in range(7)]
        live = jnp.zeros((robots, LANES), jnp.float32)
        for j in range(per):
            count = jnp.broadcast_to(counts[:, k * per + j : k * per + j + 1], live.shape)
            live = jnp.where((lane >= j * block) & (lane < j * block + count), 1.0, live)
        ids = field[6].astype(jnp.int32) + side
        sums = slot_sums(field, live, ids, wide)
        tables = []
        for v in range(3):
            start = 7 * rows + v * owned_rows
            lines = [
                recv_ref[pl.ds(at[k * per + j] * height + start, owned_rows), :]
                for j in range(per)
            ]
            old = jnp.concatenate(lines, axis=0)
            new = (old + sums[v]) / (1.0 + sums[3])
            for j in range(per):
                news_ref[v, k * per + j] = new[j * owned_rows : (j + 1) * owned_rows]
            change = new - old
            dual = dual + sums[3] * change * change
            tables.append([new[j : j + 1] for j in range(wide)])
        back = lookup(tables, ids, robots)
        for v in range(3):
            backs_ref[v, pl.ds(k * robots, robots), :] = back[v]
            differ = (field[v] - back[v]) * live
            primal = primal + differ * differ
    me = lax.axis_index("robot")
    mine = sum(jnp.where(me == r, at[r], 0) for r in range(robots))
    for v in range(3):
        back_ref[v] = backs_ref[v, pl.ds(mine, rows, robots), :]
        consensus_ref[v] = news_ref[v, me]
    write_sending(pose_ref, primal, dual, out_ref)


def pack_blocks_kernel(block, counts_ref, copies_ref, duals_ref, ids_ref, out_ref, live_ref):
    rows = ids_ref.shape[0]
    per = LANES // block
    lane = lax.broadcasted_iota(jnp.int32, (rows, LANES), 1)
    sources = [copies_ref[k] for k in range(3)] + [duals_ref[k] for k in range(3)]
    sources.append(ids_ref[...].astype(jnp.float32))
    mask = jnp.zeros((rows, LANES), jnp.float32)
    for j in range(per):
        for v, source in enumerate(sources):
            moved = pltpu.roll(source, LANES - j * block, 1) if j else source
            out_ref[pl.ds(j * FIELDS + v, rows, per * FIELDS), :] = moved
        count = column_of(counts_ref, j, per, rows)
        live = (lane < count).astype(jnp.float32)
        out_ref[pl.ds(j * FIELDS + 7, rows, per * FIELDS), :] = live
        here = (lane >= j * block) & (lane < j * block + count)
        mask = jnp.where(here, 1.0, mask)
    live_ref[...] = mask


def owner_kernel(block, recv_ref, old_ref, consensus_ref, out_ref):
    robots = recv_ref.shape[0] // FIELDS
    rows = old_ref.shape[1]
    field = [recv_ref[pl.ds(v, robots, FIELDS), :] for v in range(FIELDS)]
    live = field[7]
    ids = field[6].astype(jnp.int32)
    sums = slot_sums(field, live, ids, max(rows, SUBLANES))
    seen = sums[3][:rows]
    dual = jnp.zeros((rows, LANES), jnp.float32)
    tables = []
    for v in range(3):
        old = old_ref[v]
        new = (old + sums[v][:rows]) / (1.0 + seen)
        consensus_ref[v] = new
        change = new - old
        dual = dual + seen * change * change
        tables.append([new[k : k + 1] for k in range(rows)])
    back = lookup(tables, ids, robots)
    primal = jnp.zeros((robots, LANES), jnp.float32)
    for v in range(3):
        differ = (field[v] - back[v]) * live
        primal = primal + differ * differ
    primal = jnp.sum(primal, axis=(0, 1), keepdims=True)
    dual = jnp.sum(dual, axis=(0, 1), keepdims=True)
    lane = lax.broadcasted_iota(jnp.int32, (robots, LANES), 1)
    partial = jnp.where(lane == block, primal, jnp.where(lane == block + 1, dual, 0.0))
    first = jnp.where(lane < block, back[0], pltpu.roll(back[1], block, 1))
    out_ref[pl.ds(0, robots, 2), :] = first
    out_ref[pl.ds(1, robots, 2), :] = jnp.where(lane < block, back[2], partial)


def collect_kernel(block, recv_ref, pose_ref, out_ref, back_ref):
    rows = back_ref.shape[1]
    per = LANES // block
    lane = lax.broadcasted_iota(jnp.int32, (rows, LANES), 1)
    back = [jnp.zeros((rows, LANES), jnp.float32) for _ in range(3)]
    for j in range(per):
        here = (lane >= j * block) & (lane < (j + 1) * block)
        for v, (line, at) in enumerate(((0, 0), (0, block), (1, 0))):
            got = recv_ref[pl.ds(2 * j + line, rows, 2 * per), :]
            turn = (j * block - at) % LANES
            moved = pltpu.roll(got, turn, 1) if turn else got
            back[v] = jnp.where(here, moved, back[v])
    for v in range(3):
        back_ref[v] = back[v]
    partial = recv_ref[pl.ds(1, rows * per, 2), :]
    lane = lax.broadcasted_iota(jnp.int32, partial.shape, 1)
    primal = jnp.where(lane == block, partial, 0.0)
    dual = jnp.where(lane == block + 1, partial, 0.0)
    write_sending(pose_ref, primal, dual, out_ref)


def observe_kernel(
    copies_ref, measured_ref, jac_ref, slot_ref, pose_ref, duals_ref, live_ref, back_ref,
    estimate_ref, self_ref, edge_ref, offset_ref, out_ref, dual_ref, consensus_ref, planes_ref,
):
    for v in range(3):
        consensus_ref[v] = estimate_ref[v]
        dual_ref[v] = duals_ref[v] + (copies_ref[v] - back_ref[v]) * live_ref[...]
    rows = slot_ref.shape[0]
    table_rows = copies_ref.shape[1]
    out_rows = out_ref.shape[1]
    for start in range(0, rows, SUBLANES):
        part = pl.ds(start, SUBLANES)
        tables = [[copies_ref[k, pl.ds(j, 1), :] for j in range(table_rows)] for k in range(3)]
        at = lookup(tables, slot_ref[part, :], SUBLANES)
        error = [measured_ref[k, part, :] - at[k] for k in range(3)]
        for a in range(6):
            pull = (
                jac_ref[a, part, :] * error[0]
                + jac_ref[6 + a, part, :] * error[1]
                + jac_ref[12 + a, part, :] * error[2]
            )
            for s, piece in enumerate(split3(pull)):
                planes_ref[s * 6 + a, part, :] = piece
    sums = segment_rows(
        lambda t: [planes_ref[j, pl.ds(t, 1), :] for j in range(18)],
        lambda t: pose_ref[pl.ds(t, 1), :],
        rows,
        out_rows,
    )
    grad = []
    for a in range(6):
        high, middle, low = (
            sums[(s * 6 + a) * out_rows : (s * 6 + a + 1) * out_rows] for s in range(3)
        )
        grad.append(high + (middle + low))
    edge = edge_ref[...]
    count = out_rows * LANES
    tables = [[self_ref[a, pl.ds(k, 1), :] for k in range(out_rows)] for a in range(6)]
    near = lookup(tables, lax.rem(edge, count), out_rows)
    here = edge // count == lax.axis_index("sub")
    for a in range(6):
        out_ref[a] = grad[a] + jnp.where(here, near[a], 0.0) - self_ref[a] - offset_ref[a]


def refine_kernel(landmark_total, edge_ref, grad_ref, inverse_ref, *refs):
    blocks, (out_ref, norm_ref) = refs[:-2], refs[-2:]
    subs = len(blocks)
    rows = edge_ref.shape[0]
    count = rows * LANES
    me = lax.axis_index("sub")
    edge = edge_ref[...]
    place = lax.bitwise_xor(edge // count, me)
    tables = [
        [held[pl.ds(a * rows + k, 1), :] for held in blocks[1:] for k in range(rows)]
        for a in range(6)
    ]
    far = lookup(tables, (place - 1) * count + lax.rem(edge, count), rows)
    far = [jnp.where(place == 0, 0.0, value) for value in far]
    own = [blocks[0][pl.ds(a * rows, rows), :] for a in range(6)]
    grad = [grad_ref[a] + far[a] for a in range(6)]
    for a in range(6):
        delta = inverse_ref[a * 6] * grad[0]
        for b in range(1, 6):
            delta = delta + inverse_ref[a * 6 + b] * grad[b]
        out_ref[a] = own[a] + delta
    total = None
    for s in range(subs):
        place = lax.bitwise_xor(me, jnp.int32(s))
        part = blocks[0][pl.ds(6 * rows, SUBLANES), :]
        for k in range(1, subs):
            part = jnp.where(place == k, blocks[k][pl.ds(6 * rows, SUBLANES), :], part)
        total = part if total is None else total + part
    norms = jnp.sqrt(jnp.sum(total, axis=1, keepdims=True) / landmark_total)
    for k in range(2):
        norm_ref[k] = norms[k, 0]


VMEM = pl.BlockSpec(memory_space=pltpu.VMEM)
SMEM = pl.BlockSpec(memory_space=pltpu.SMEM)


def vmem(*shape):
    return pltpu.VMEM(shape, jnp.float32)


TRIED_ORDERS = {8: (5, 3, 0, 7, 6, 2, 1, 4)}


def meeting_order(robots):
    first = robots * 3 // 4
    rest = [i for i in range(robots) if i != first]
    return list(TRIED_ORDERS.get(robots, [first] + rest))


def over_robots(value, robots, order=None):
    blocks = value.reshape(robots, 1, value.shape[0] // robots * LANES)
    groups = None if order is None else [list(order)]
    moved = lax.all_to_all(blocks, "robot", 0, 0, tiled=True, axis_index_groups=groups)
    return moved.reshape(value.shape)


def in_vmem(value):
    return pltpu.with_memory_space_constraint(value, pltpu.VMEM)


def call(kernel, outs, in_specs, out_specs=None, scratch=()):
    shapes = [
        jax.ShapeDtypeStruct(shape, jnp.float32) if isinstance(shape, tuple) else shape
        for shape in outs
    ]
    return pl.pallas_call(
        kernel,
        out_shape=shapes,
        in_specs=in_specs,
        out_specs=out_specs or [VMEM] * len(outs),
        scratch_shapes=list(scratch),
    )


def step(
    landmark_copies,
    dual_copies,
    visibility,
    block_counts,
    consensus_old,
    poses,
    inverse_blocks,
    jacobians,
    measurements,
    obs_pose,
    obs_slot,
    edge_to,
    edge_offset,
):
    robots = lax.axis_size("robot")
    subs = lax.axis_size("sub")
    slots = landmark_copies.shape[3]
    owned = consensus_old.shape[3]
    pose_count = poses.shape[3]
    observed = obs_slot.shape[2]
    block = slots // robots
    rows, owned_rows = slots // LANES, owned // LANES
    pose_rows, obs_rows = pose_count // LANES, observed // LANES

    copies = landmark_copies.reshape(3, rows, LANES)
    duals = dual_copies.reshape(3, rows, LANES)
    ids = visibility.reshape(rows, LANES)
    counts = block_counts.reshape(1, robots)
    old = consensus_old.reshape(3, owned_rows, LANES)
    pose_block = poses.reshape(6, pose_rows, LANES)
    inverse = inverse_blocks.reshape(36, pose_rows, LANES)
    jac = jacobians.reshape(18, obs_rows, LANES)
    measured = measurements.reshape(3, obs_rows, LANES)
    pose_ids = obs_pose.reshape(obs_rows, LANES)
    slot_ids = obs_slot.reshape(obs_rows, LANES)
    edges = edge_to.reshape(pose_rows, LANES)
    offset = edge_offset.reshape(6, pose_rows, LANES)

    height = block_rows(robots, rows, owned_rows)
    sending_rows = 6 * pose_rows + SUBLANES
    if robots * height * LANES * 4 <= WHOLE_BYTES:
        outgoing, live, copies, duals, edges = call(
            functools.partial(pack_kernel, block),
            [vmem(robots * height, LANES), vmem(rows, LANES)]
            + [vmem(3, rows, LANES)] * 2
            + [pltpu.VMEM((pose_rows, LANES), jnp.int32)],
            [SMEM] + [VMEM] * 5,
        )(counts, copies, duals, ids, old, edges)
        order = meeting_order(robots)
        received = over_robots(outgoing, robots, order)
        sending, back, estimate = call(
            functools.partial(consensus_kernel, block, owned_rows, order),
            [vmem(sending_rows, LANES), vmem(3, rows, LANES), vmem(3, owned_rows, LANES)],
            [VMEM] * 2,
            scratch=[vmem(3, rows * robots, LANES), vmem(3, robots, owned_rows, LANES)],
        )(in_vmem(received), in_vmem(pose_block))
    else:
        outgoing, live = call(
            functools.partial(pack_blocks_kernel, block),
            [vmem(robots * FIELDS, LANES), vmem(rows, LANES)],
            [SMEM, VMEM, VMEM, VMEM],
        )(counts, copies, duals, ids)
        received = over_robots(outgoing, robots)
        estimate, returning = call(
            functools.partial(owner_kernel, block),
            [vmem(3, owned_rows, LANES), vmem(robots * 2, LANES)],
            [VMEM] * 2,
        )(in_vmem(received), in_vmem(old))
        sending, back = call(
            functools.partial(collect_kernel, block),
            [vmem(sending_rows, LANES), vmem(3, rows, LANES)],
            [VMEM] * 2,
        )(in_vmem(over_robots(returning, robots)), in_vmem(pose_block))

    held = [sending]
    for k in range(1, subs):
        ring = [(i, i ^ k) for i in range(subs)]
        held.append(lax.ppermute(sending, "sub", ring))

    grad_obs, dual_new, consensus = call(
        observe_kernel,
        [vmem(6, pose_rows, LANES), (3, rows, LANES), (3, owned_rows, LANES)],
        [VMEM] * 12,
        scratch=[pltpu.VMEM((18, obs_rows, LANES), jnp.float32)],
    )(
        in_vmem(copies),
        in_vmem(measured),
        in_vmem(jac),
        in_vmem(slot_ids),
        in_vmem(pose_ids),
        in_vmem(duals),
        in_vmem(live),
        in_vmem(back),
        in_vmem(estimate),
        in_vmem(pose_block),
        in_vmem(edges),
        in_vmem(offset),
    )

    refined, residual_norms = call(
        functools.partial(refine_kernel, float(owned * robots * subs)),
        [(6, pose_rows, LANES), (2,)],
        [VMEM] * (3 + subs),
        out_specs=[VMEM, SMEM],
    )(
        in_vmem(edges),
        in_vmem(grad_obs),
        in_vmem(inverse),
        *[in_vmem(value) for value in held],
    )
    return (
        refined.reshape(1, 1, 6, pose_count),
        consensus.reshape(1, 1, 3, owned),
        dual_new.reshape(1, 1, 3, slots),
        residual_norms,
    )


def solution(mesh):
    split4 = P("robot", "sub", None, None)
    split3d = P("robot", "sub", None)
    return jax.shard_map(
        step,
        mesh=mesh,
        in_specs=(
            split4,
            split4,
            split3d,
            split3d,
            split4,
            split4,
            split4,
            split4,
            split4,
            split3d,
            split3d,
            split3d,
            split4,
        ),
        out_specs=(split4, split4, split4, P()),
        check_vma=False,
    )
```
